512 devices in a mesh: gx: 32 (over z, y_hi, core), gy: 16 (over y_lo, x).
Axes of the slice: x: 4, y: 8 (y_hi: 2, y_lo: 4; y = y_hi * 4 + y_lo), z: 8, core: 2. Of those that a mesh axis runs over, the one named last changes fastest.
Arguments:
- hidden70: bfloat16 [32, 8192], P('gx', 'gy'), may hold values from -6 to 6
- attn_gain: float32 [8192], P('gy'), may hold values from 0.5 to 1.5
- final_gain: float32 [8192], P('gy'), may hold values from 0.5 to 1.5
- query_weight: bfloat16 [8192, 8192], P('gy', 'gx'), may hold values from -0.0625 to 0.0625
- keyvalue_weight: bfloat16 [8192, 2048], P('gy', 'gx'), may hold values from -0.0625 to 0.0625
- out_weight: bfloat16 [8192, 8192], P('gx', 'gy'), may hold values from -0.0625 to 0.0625
- key_cache: bfloat16 [32, 256, 1024], P('gy', 'gx'), may hold values from -444 to 444
- value_cache: bfloat16 [32, 256, 1024], P('gy', 'gx'), may hold values from -6 to 6
- lengths: int32 [32], P('gy'), may hold values from 2 to 256
- head70: bfloat16 [8192, 32000], P('gy', 'gx'), may hold values from -2 to 2
- adjusted_hidden: bfloat16 [32, 4096], P('gx', 'gy'), may hold values from -4 to 4
- adjusted_gain: float32 [4096], P('gy'), may hold values from 0.5 to 1.5
- adjusted_head: bfloat16 [4096, 32000], P('gy', 'gx'), may hold values from -3 to 3
- base_hidden: bfloat16 [32, 4096], P('gx', 'gy'), may hold values from -6 to 6
- base_gain: float32 [4096], P('gy'), may hold values from 0.5 to 1.5
- base_head: bfloat16 [4096, 32000], P('gy', 'gx'), may hold values from -3 to 3
Outputs:
- log_probs: float32 [32, 32000], P('gy', 'gx')
The draws below stay inside these ranges and needn't reach their ends.
Inputs may be any that keep to these rules, and one draw needn't show every extreme that they name: Row r has valid cache slots 0 to lengths[r] - 1 and its new token stands at position lengths[r].
All inputs are finite; a program needn't handle non-finite values.
Results may differ from the reference program's by a relative error of at most 0.00065.
Values may be sent and summed in bfloat16 or wider, within the bound.
A program may use at most 64 MiB of HBM per device.

```python
import jax
import jax.numpy as jnp
from jax import lax

D = 8192
HEADS = 64
KV_HEADS = 8
HEAD_DIM = 128
D7 = 4096
VOCAB = 32000
CTX = 256
ROWS = 32


def base_field(key, shape):
    return jnp.clip(jax.random.normal(key, shape, jnp.float32), -4.0, 4.0)


def row_strength(key, levels):
    order = jax.random.permutation(key, ROWS)
    picks = order % 4
    return jnp.asarray(levels, jnp.float32)[picks]


def vocab_plan(key):
    levels = (0.0, 90.0, 170.0, 260.0)
    strength = row_strength(jax.random.fold_in(key, 31), levels)
    columns = jax.random.permutation(jax.random.fold_in(key, 32), VOCAB)[:2 * ROWS]
    first = columns[:ROWS]
    second = columns[ROWS:]
    spacing = jax.random.uniform(jax.random.fold_in(key, 33), (ROWS,), jnp.float32, 1.3, 2.7)
    direction = base_field(jax.random.fold_in(key, 34), (ROWS, D7))
    return (strength, first, second, spacing, direction)


def draw_key_cache(key, part):
    width = KV_HEADS * HEAD_DIM
    cache = base_field(jax.random.fold_in(key, 21), (ROWS, CTX, width))
    strength = row_strength(jax.random.fold_in(key, 22), (0.0, 40.0, 85.0, 110.0))
    direction = base_field(jax.random.fold_in(key, 23), (ROWS, width))
    planted = (jnp.arange(CTX, dtype=jnp.int32) < 2).astype(jnp.float32)
    result = cache + strength[:, None, None] * planted[None, :, None] * direction[:, None, :]
    return result.astype(jnp.bfloat16)


def draw_adjusted_hidden(key, part):
    strength, first, second, spacing, direction = vocab_plan(key)
    return direction.astype(jnp.bfloat16)


def draw_adjusted_head(key, part):
    strength, first, second, spacing, direction = vocab_plan(key)
    scale = (D7 // 9) ** (-0.5)
    table = base_field(jax.random.fold_in(key, 41), (D7, VOCAB)) * scale
    noise = base_field(jax.random.fold_in(key, 42), (2 * ROWS, D7)) * scale
    spread = jnp.maximum(jnp.sqrt(jnp.mean(direction * direction, axis=1)), 0.5)
    unit = direction / (spread[:, None] * D7)
    col_first = strength[:, None] * unit + 0.05 * noise[:ROWS]
    col_second = (strength - spacing)[:, None] * unit + 0.05 * noise[ROWS:]
    live = (strength > 0.0)[:, None]
    col_first = jnp.where(live, col_first, table[:, first].T)
    col_second = jnp.where(live, col_second, table[:, second].T)
    table = table.at[:, first].set(col_first.T)
    table = table.at[:, second].set(col_second.T)
    return table.astype(jnp.bfloat16)


def draw_head70(key, part):
    strength, first, second, spacing, direction = vocab_plan(key)
    scale = (D // 9) ** (-0.5)
    table = base_field(jax.random.fold_in(key, 51), (D, VOCAB)) * scale
    noise = base_field(jax.random.fold_in(key, 52), (D, ROWS)) * scale
    copied = table[:, first] + 0.05 * noise
    live = (strength > 0.0)[None, :]
    table = table.at[:, second].set(jnp.where(live, copied, table[:, second]))
    return table.astype(jnp.bfloat16)


def draw_base_head(key, part):
    strength, first, second, spacing, direction = vocab_plan(key)
    scale = (D7 // 9) ** (-0.5)
    table = base_field(jax.random.fold_in(key, 61), (D7, VOCAB)) * scale
    noise = base_field(jax.random.fold_in(key, 62), (D7, ROWS)) * scale
    copied = table[:, first] + 0.05 * noise
    live = (strength > 0.0)[None, :]
    table = table.at[:, second].set(jnp.where(live, copied, table[:, second]))
    return table.astype(jnp.bfloat16)


def touch_ends(values, own_key, smallest, high):
    extent = values.shape
    index_at = [jax.random.randint(jax.random.fold_in(own_key, axis), (), 0, extent[axis]) for axis in range(len(extent))]
    values = values.at[tuple(index_at)].set(smallest)
    longest = extent.index(max(extent))
    index_at[longest] = (index_at[longest] + 1) % extent[longest]
    return values.at[tuple(index_at)].set(high)


def shard_levels(own_key, dims, shards, low, top_value):
    def one(axis_at, blocks):
        heights = jax.random.uniform(jax.random.fold_in(jax.random.fold_in(own_key, 6), axis_at), (blocks,), jnp.float32, low / len(shards), top_value / len(shards))
        return jnp.repeat(jnp.exp(heights), dims[axis_at] // blocks).reshape((-1,) + (1,) * (len(dims) - axis_at - 1))

    level = one(*shards[0])
    for cut in shards[1:]:
        level = level * one(*cut)
    return level


def scatter_about(own_key, shape, scale, reach, shards=(), held_as=jnp.bfloat16):
    entries = jax.random.normal(own_key, shape, jnp.float32) * scale
    if len(shards) > 0:
        entries = shard_levels(own_key, shape, shards, -0.22, 0.18) * entries
    return jnp.clip(entries, min=-reach, max=reach).astype(held_as)


def setup_inputs(seed: int = 0) -> dict:
    arg_keys = jax.random.split(jax.random.key(seed), 17)
    return {
        "hidden70": scatter_about(arg_keys[0], (ROWS, D), 1.0, 6.0, ((0, 32), (1, 16))),
        "attn_gain": jnp.clip(1.0 + 0.1 * jax.random.normal(arg_keys[1], (D,), jnp.float32), 0.5, 1.5),
        "final_gain": jnp.clip(1.0 + 0.1 * jax.random.normal(arg_keys[2], (D,), jnp.float32), 0.5, 1.5),
        "query_weight": scatter_about(arg_keys[3], (D, D), D ** -0.5, 0.0625, ((0, 16), (1, 32))),
        "keyvalue_weight": scatter_about(arg_keys[4], (D, 2 * KV_HEADS * HEAD_DIM), D ** -0.5, 0.0625, ((0, 16), (1, 32))),
        "out_weight": scatter_about(arg_keys[5], (D, D), D ** -0.5, 0.0625, ((0, 32), (1, 16))),
        "key_cache": draw_key_cache(jax.random.fold_in(arg_keys[16], 71), 0),
        "value_cache": scatter_about(arg_keys[7], (ROWS, CTX, KV_HEADS * HEAD_DIM), 1.0, 6.0, ((0, 16), (1, 32))),
        "lengths": touch_ends(jax.random.randint(arg_keys[8], (ROWS,), 2, CTX + 1), jax.random.fold_in(arg_keys[8], 1), 2, CTX).astype(jnp.int32),
        "head70": draw_head70(jax.random.fold_in(arg_keys[16], 71), 0),
        "adjusted_hidden": draw_adjusted_hidden(jax.random.fold_in(arg_keys[16], 71), 0),
        "adjusted_gain": jnp.clip(1.0 + 0.1 * jax.random.normal(arg_keys[11], (D7,), jnp.float32), 0.5, 1.5),
        "adjusted_head": draw_adjusted_head(jax.random.fold_in(arg_keys[16], 71), 0),
        "base_hidden": scatter_about(arg_keys[13], (ROWS, D7), 1.0, 6.0, ((0, 32), (1, 16))),
        "base_gain": jnp.clip(1.0 + 0.1 * jax.random.normal(arg_keys[14], (D7,), jnp.float32), 0.5, 1.5),
        "base_head": draw_base_head(jax.random.fold_in(arg_keys[16], 71), 0),
    }


EPS = 1e-05
THETA = 10000.0

def rotate(values, positions):
    width = values.shape[-1]
    half = width // 2
    freq = THETA ** (-(jnp.arange(half, dtype=jnp.float32) * 2.0 / width))
    angle = positions.astype(jnp.float32)[:, None] * freq[None, :]
    cosine = jnp.cos(angle)[:, None, :]
    sine = jnp.sin(angle)[:, None, :]
    first = values[..., :half]
    second = values[..., half:]
    return jnp.concatenate([first * cosine - second * sine, second * cosine + first * sine], axis=-1)

def norm_rows(values, gain):
    return values * lax.rsqrt(lax.optimization_barrier(jnp.mean(values * values, axis=1, keepdims=True)) + EPS) * gain

def reference(hidden70, attn_gain, final_gain, query_weight, keyvalue_weight, out_weight, key_cache, value_cache, lengths, head70, adjusted_hidden, adjusted_gain, adjusted_head, base_hidden, base_gain, base_head):
    resid_in = hidden70.astype(jnp.float32)
    normed = norm_rows(resid_in, attn_gain).astype(jnp.bfloat16)
    q_linear = jnp.dot(normed, query_weight, preferred_element_type=jnp.float32).astype(jnp.bfloat16)
    kv_linear = jnp.dot(normed, keyvalue_weight, preferred_element_type=jnp.float32).astype(jnp.bfloat16)
    count = hidden70.shape[0]
    kv_width = KV_HEADS * HEAD_DIM
    group = HEADS // KV_HEADS
    query = rotate(q_linear.astype(jnp.float32).reshape(count, HEADS, HEAD_DIM), lengths).astype(jnp.bfloat16)
    key_new = rotate(kv_linear[:, :kv_width].astype(jnp.float32).reshape(count, KV_HEADS, HEAD_DIM), lengths).astype(jnp.bfloat16)
    value_new = kv_linear[:, kv_width:].reshape(count, KV_HEADS, HEAD_DIM)
    scale = HEAD_DIM ** (-0.5)
    query_four = query.astype(jnp.float32).reshape(count, KV_HEADS, group, HEAD_DIM)
    keys = key_cache.astype(jnp.float32).reshape(count, CTX, KV_HEADS, HEAD_DIM)
    values = value_cache.astype(jnp.float32).reshape(count, CTX, KV_HEADS, HEAD_DIM)
    scores = jnp.einsum('rkgd,rtkd->rkgt', query_four, keys) * scale
    valid = (jnp.arange(CTX, dtype=jnp.int32)[None, :] < lengths[:, None])[:, None, None, :]
    scores = jnp.where(valid, scores, -jnp.inf)
    fresh_score = jnp.einsum('rkgd,rkd->rkg', query_four, key_new.astype(jnp.float32)) * scale
    largest = jnp.maximum(lax.optimization_barrier(jnp.max(scores, axis=-1)), fresh_score)
    weights = jnp.exp(scores - largest[..., None])
    fresh = jnp.exp(fresh_score - largest)
    total = lax.optimization_barrier(jnp.sum(weights, axis=-1)) + fresh
    summed = jnp.einsum('rkgt,rtkd->rkgd', weights.astype(jnp.bfloat16).astype(jnp.float32), values)
    summed = summed + fresh.astype(jnp.bfloat16).astype(jnp.float32)[..., None] * value_new.astype(jnp.float32)[:, :, None, :]
    attn = (summed / total[..., None]).reshape(count, HEADS * HEAD_DIM).astype(jnp.bfloat16)
    resid = resid_in + jnp.dot(attn, out_weight, preferred_element_type=jnp.float32)
    final = norm_rows(resid, final_gain).astype(jnp.bfloat16)
    adjusted = norm_rows(adjusted_hidden.astype(jnp.float32), adjusted_gain).astype(jnp.bfloat16)
    base = norm_rows(base_hidden.astype(jnp.float32), base_gain).astype(jnp.bfloat16)
    logits = jnp.dot(final, head70, preferred_element_type=jnp.float32)
    logits = logits + jnp.dot(adjusted, adjusted_head, preferred_element_type=jnp.float32)
    logits = logits - jnp.dot(base, base_head, preferred_element_type=jnp.float32)
    peak = lax.optimization_barrier(jnp.max(logits, axis=1, keepdims=True))
    return logits - peak - jnp.log(lax.optimization_barrier(jnp.sum(jnp.exp(logits - peak), axis=1, keepdims=True)))
```

```python
import functools
import math

import jax
import jax.numpy as jnp
from jax import lax
from jax.experimental import pallas as pl
from jax.experimental.pallas import tpu as pltpu
from jax.sharding import PartitionSpec as P

D = 8192
HEADS = 64
KV_HEADS = 8
HEAD_DIM = 128
D7 = 4096
CTX = 256

EPS = 1e-05
THETA = 10000.0
NEGATIVE = -1e30

GX = 32
GY = 16
MESH = pl.DeviceIdType.MESH
BF = jnp.bfloat16
F32 = jnp.float32


def times_transposed(a, b):
    return lax.dot_general(a, b, (((1,), (1,)), ((), ())), preferred_element_type=F32)


def kernel(
    lengths,
    hidden,
    attn_gain,
    final_gain,
    query_weight,
    keyvalue_weight,
    out_weight,
    key_cache,
    value_cache,
    head70,
    adjusted_hidden,
    adjusted_gain,
    adjusted_head,
    base_hidden,
    base_gain,
    base_head,
    out,
    hid_v,
    ag_v,
    fg_v,
    qw_v,
    kvw_v,
    ow_v,
    kv_v,
    h70_v,
    ah_v,
    agn_v,
    ahead_v,
    bh_v,
    bgn_v,
    bhead_v,
    x_send,
    x_recv,
    st_send,
    st_recv,
    cache_recv,
    ab_send,
    ab_recv,
    q_send,
    q_recv,
    kn_send,
    kn_recv,
    e_send,
    e_recv,
    f_send,
    f_recv,
    h_send,
    h_recv,
    abl_send,
    abl_recv,
    i_send,
    i_recv,
    j_send,
    j_recv,
    load_sem,
    send_sem,
    recv_sem,
    entered,
):
    gx = lax.axis_index("gx")
    gy = lax.axis_index("gy")
    z = gx // 4
    yh = (gx // 2) % 2
    core = gx % 2
    row = 2 * gy + yh

    pairs = [
        (hidden, hid_v),
        (adjusted_hidden, ah_v),
        (base_hidden, bh_v),
        (adjusted_gain, agn_v),
        (base_gain, bgn_v),
        (attn_gain, ag_v),
        (key_cache, kv_v.at[0]),
        (value_cache, kv_v.at[1]),
        (query_weight, qw_v),
        (keyvalue_weight, kvw_v),
        (out_weight, ow_v),
        (adjusted_head, ahead_v),
        (base_head, bhead_v),
        (final_gain, fg_v),
        (head70, h70_v),
    ]
    loads = [
        pltpu.make_async_copy(src, dst, load_sem.at[n]) for n, (src, dst) in enumerate(pairs)
    ]
    for load in loads:
        load.start()
    own_cache = [
        pltpu.make_async_copy(
            src.at[yh, :, pl.ds(pl.multiple_of(z * HEAD_DIM, HEAD_DIM), HEAD_DIM)],
            cache_recv.at[gx, n],
            load_sem.at[len(pairs) + n],
        )
        for n, src in enumerate((key_cache, value_cache))
    ]
    for load in own_cache:
        load.start()

    def over_gx(act):
        lax.fori_loop(1, GX, lambda k, c: (act(lax.rem(gx + k, GX)), c)[1], 0)

    def over_gy(act):
        lax.fori_loop(1, GY, lambda k, c: (act(lax.rem(gy + k, GY)), c)[1], 0)

    def send(n, src, dst, to):
        pltpu.make_async_remote_copy(
            src_ref=src,
            dst_ref=dst,
            send_sem=send_sem.at[n],
            recv_sem=recv_sem.at[n],
            device_id=to,
            device_id_type=MESH,
        ).start()

    def arrived(n, ref):
        pltpu.make_async_copy(ref, ref, recv_sem.at[n]).wait()

    def sent(n, ref):
        pltpu.make_async_copy(ref, ref, send_sem.at[n]).wait()

    barrier = pltpu.get_barrier_semaphore()
    over_gx(
        lambda t: pl.semaphore_signal(barrier, inc=1, device_id=(t, gy), device_id_type=MESH)
    )
    over_gy(
        lambda t: pl.semaphore_signal(barrier, inc=1, device_id=(gx, t), device_id_type=MESH)
    )

    def as_tiles(x, width):
        return [x[:, n * 128 : (n + 1) * 128] for n in range(width // 128)]

    loads[0].wait()
    own_x = jnp.concatenate(as_tiles(hid_v[...].astype(F32), 512), axis=0)
    x_send[...] = own_x.astype(BF)
    x_recv[gx] = x_send[...]
    loads[1].wait()
    loads[2].wait()
    adjusted_in = ah_v[...].astype(F32)
    base_in = bh_v[...].astype(F32)
    sum_adjusted = jnp.sum(adjusted_in * adjusted_in, axis=1, keepdims=True)
    sum_base = jnp.sum(base_in * base_in, axis=1, keepdims=True)
    st_send[...] = jnp.concatenate(
        [jnp.broadcast_to(sum_adjusted, (1, 128)), jnp.broadcast_to(sum_base, (1, 128))], axis=0
    )
    st_recv[gy] = st_send[...]

    pl.semaphore_wait(barrier, GX - 1 + GY - 1)

    over_gx(lambda t: send(0, x_send, x_recv.at[gx], (t, gy)))
    over_gy(
        lambda t: pl.semaphore_signal(entered, inc=1, device_id=(gx, t), device_id_type=MESH)
    )
    over_gy(lambda t: send(1, st_send, st_recv.at[gy], (gx, t)))
    loads[6].wait()
    loads[7].wait()

    def send_cache(t):
        head = pl.multiple_of((t // 4) * HEAD_DIM, HEAD_DIM)
        send(
            2,
            kv_v.at[:, (t // 2) % 2, :, pl.ds(head, HEAD_DIM)],
            cache_recv.at[gx],
            (t, gy),
        )

    over_gx(send_cache)

    lane = lax.broadcasted_iota(jnp.int32, (1, HEAD_DIM), 1)
    half = HEAD_DIM // 2
    pair = (lane % half).astype(F32)
    freq = jnp.exp(pair * (-2.0 / HEAD_DIM * math.log(THETA)))
    length = lengths[yh]
    angle = length.astype(F32) * freq
    cosine = jnp.cos(angle)
    sine = jnp.where(lane < half, -jnp.sin(angle), jnp.sin(angle))

    loads[5].wait()
    loads[8].wait()
    loads[9].wait()

    def from_tiles(x):
        return jnp.concatenate([x[:, n, :] for n in range(4)], axis=1)

    arrived(0, x_recv.at[pl.ds(0, GX - 1)])
    rows = from_tiles(x_recv[...].astype(F32))
    squares = jnp.sum(rows * rows, axis=1, keepdims=True)
    scaled = (rows * ag_v[...]).astype(BF)
    part_q = jnp.dot(scaled, qw_v[...], preferred_element_type=F32)
    part_kv = times_transposed(scaled, kvw_v[...])
    high = squares.astype(BF).astype(F32)
    low = squares - high
    pieces = [
        part_q[:, :128],
        part_q[:, 128:],
        jnp.broadcast_to(high, (GX, 128)),
        jnp.broadcast_to(low, (GX, 128)),
    ]
    q_send[...] = jnp.concatenate([p.reshape(GX, 1, 128) for p in pieces], axis=1).astype(BF)
    nothing = jnp.zeros_like(part_kv)
    wide = jnp.where(
        core == 0,
        jnp.concatenate([part_kv, nothing], axis=1),
        jnp.concatenate([nothing, part_kv], axis=1),
    )
    kn_send[...] = wide.reshape(GX, 1, 128)
    q_recv[row] = q_send[row]

    pl.semaphore_wait(entered, GY - 1)

    def send_q(k, c):
        r = lax.rem(row + k, GX)
        send(3, q_send.at[r], q_recv.at[row], (4 * z + 2 * (r % 2) + core, r // 2))
        return c

    lax.fori_loop(1, GX, send_q, 0)
    kind = z // 4
    head_to = (2 * z + yh) % KV_HEADS
    meets_itself = head_to == z
    slot = (kind * 2 + core) * GY + gy

    def send_kn(k, c):
        r = k // 2
        to = 4 * head_to + 2 * (r % 2) + k % 2
        itself = jnp.logical_and(to == gx, r // 2 == gy)

        @pl.when(itself)
        def _():
            kn_recv[slot] = kn_send[r]

        @pl.when(jnp.logical_not(itself))
        def _():
            send(4, kn_send.at[r], kn_recv.at[slot], (to, r // 2))

        return c

    lax.fori_loop(0, 2 * GX, send_kn, 0)

    def without_own(act):
        @pl.when(meets_itself)
        def _():
            act(4, kn_recv.at[pl.ds(0, 4 * GY - 1)])

        @pl.when(jnp.logical_not(meets_itself))
        def _():
            act(4, kn_recv)

    arrived(1, st_recv.at[pl.ds(0, GY - 1)])
    totals = jnp.sum(st_recv[...], axis=0)
    loads[3].wait()
    loads[4].wait()
    adjusted = adjusted_in * lax.rsqrt(totals[0:1, 0:1] / D7 + EPS) * agn_v[...]
    base = base_in * lax.rsqrt(totals[1:2, 0:1] / D7 + EPS) * bgn_v[...]
    ab_send[...] = jnp.concatenate(as_tiles(adjusted, 256) + as_tiles(base, 256), axis=0).astype(BF)
    ab_recv[gx] = ab_send[...]
    over_gx(lambda t: send(5, ab_send, ab_recv.at[gx], (t, gy)))

    for load in own_cache:
        load.wait()
    arrived(2, cache_recv.at[pl.ds(0, GX - 1)])
    cached = cache_recv[...].astype(F32)
    keys = cached[:, 0].reshape(CTX, HEAD_DIM).astype(BF)
    values = cached[:, 1].reshape(CTX, HEAD_DIM).astype(BF)

    arrived(3, q_recv.at[pl.ds(0, GX - 1)])
    without_own(arrived)

    q_total = jnp.zeros((2, 4, 128), F32)
    for n in range(GY):
        q_total = q_total + q_recv[2 * n : 2 * n + 2].astype(F32)
    square = q_total[0, 2:3, :] + q_total[0, 3:4, :]
    factor = lax.rsqrt(square / D + EPS)
    query = jnp.concatenate([q_total[0, 0:2, :], q_total[1, 0:2, :]], axis=0) * factor
    query = query.astype(BF).astype(F32)
    fresh_kv = kn_recv[...]
    key_new = (jnp.sum(fresh_kv[: 2 * GY], axis=0) * factor).astype(BF).astype(F32)
    value_new = (jnp.sum(fresh_kv[2 * GY :], axis=0) * factor).astype(BF).astype(F32)
    scale = HEAD_DIM ** (-0.5)
    fresh_score = jnp.sum(query * key_new, axis=1, keepdims=True) * scale
    turned = (query * cosine + pltpu.roll(query, half, 1) * sine).astype(BF)
    scores = times_transposed(turned, keys) * scale
    position = lax.broadcasted_iota(jnp.int32, (4, CTX), 1)
    valid = position < length
    scores = jnp.where(valid, scores, NEGATIVE)
    top = jnp.maximum(jnp.max(scores, axis=1, keepdims=True), fresh_score)
    weights = jnp.where(valid, jnp.exp(scores - top), 0.0)
    fresh = jnp.exp(fresh_score - top)
    total = jnp.sum(weights, axis=1, keepdims=True) + fresh
    summed = jnp.dot(weights.astype(BF), values, preferred_element_type=F32)
    summed = summed + fresh.astype(BF).astype(F32) * value_new
    attn = (summed / total).astype(BF)
    e_send[0] = attn[0:2]
    e_send[1] = attn[2:4]
    e_recv[row] = e_send[yh]

    def send_e(k, c):
        r = lax.rem(row + k, GX)
        to = r % 2
        send(6, e_send.at[to], e_recv.at[row], (4 * z + 2 * to + core, r // 2))
        return c

    lax.fori_loop(1, GX, send_e, 0)

    arrived(5, ab_recv.at[pl.ds(0, GX - 1)])
    joined = from_tiles(ab_recv[...].astype(F32)).astype(BF)
    loads[11].wait()
    loads[12].wait()
    part_ab = times_transposed(joined[:, :256], ahead_v[...]) - times_transposed(
        joined[:, 256:], bhead_v[...]
    )
    vocab = part_ab.shape[1]
    for n in range(GY):
        abl_send[n] = part_ab[2 * n : 2 * n + 2]
    abl_recv[gy] = abl_send[gy]
    over_gy(lambda t: send(7, abl_send.at[t], abl_recv.at[gy], (gx, t)))

    loads[10].wait()
    arrived(6, e_recv.at[pl.ds(0, GX - 1)])
    heads = e_recv[...].astype(F32)
    heads = jnp.concatenate([heads[:, 0, :], heads[:, 1, :]], axis=1).astype(BF)
    mixed = jnp.dot(heads, ow_v[...], preferred_element_type=F32)
    f_send[...] = jnp.concatenate(
        [p.reshape(GX, 1, 128) for p in as_tiles(mixed, 512)], axis=1
    ).astype(BF)
    f_recv[gx] = f_send[gx]

    over_gx(lambda t: send(8, f_send.at[t], f_recv.at[gx], (t, gy)))
    arrived(7, abl_recv.at[pl.ds(0, GY - 1)])
    ab_logits = jnp.sum(abl_recv[...], axis=0)
    loads[13].wait()
    loads[14].wait()
    arrived(8, f_recv.at[pl.ds(0, GX - 1)])
    resid = own_x + jnp.sum(f_recv[...].astype(F32), axis=0)

    h_send[...] = resid.astype(BF)
    h_recv[gx] = h_send[...]
    over_gx(lambda t: send(9, h_send, h_recv.at[gx], (t, gy)))
    arrived(9, h_recv.at[pl.ds(0, GX - 1)])
    rows = from_tiles(h_recv[...].astype(F32))
    squares = jnp.sum(rows * rows, axis=1, keepdims=True)
    scaled = (rows * fg_v[...]).astype(BF)
    part = times_transposed(scaled, h70_v[...])
    square = jnp.broadcast_to(squares, (GX, 128))
    for n in range(GY):
        i_send[n, :, :vocab] = part[2 * n : 2 * n + 2]
        i_send[n, :, 1024:] = square[2 * n : 2 * n + 2]
    i_recv[gy] = i_send[gy]

    over_gy(lambda t: send(10, i_send.at[t], i_recv.at[gy], (gx, t)))
    arrived(10, i_recv.at[pl.ds(0, GY - 1)])
    summed = jnp.sum(i_recv[...], axis=0)
    factor = lax.rsqrt(summed[:, 1024:1025] / D + EPS)
    logits = summed[:, :vocab] * factor + ab_logits
    peak = jnp.max(logits, axis=1, keepdims=True)
    partial_lse = peak + jnp.log(jnp.sum(jnp.exp(logits - peak), axis=1, keepdims=True))
    j_send[...] = jnp.broadcast_to(partial_lse, (2, 128))
    j_recv[gx] = j_send[...]

    over_gx(lambda t: send(11, j_send, j_recv.at[gx], (t, gy)))
    arrived(11, j_recv.at[pl.ds(0, GX - 1)])
    everyone = j_recv[...]
    peak = jnp.max(everyone, axis=0)
    lse = peak + jnp.log(jnp.sum(jnp.exp(everyone - peak[None]), axis=0))
    out[...] = logits - lse[:, 0:1]

    sent(0, x_recv.at[pl.ds(0, GX - 1)])
    sent(1, st_recv.at[pl.ds(0, GY - 1)])
    sent(2, cache_recv.at[pl.ds(0, GX - 1)])
    sent(3, q_recv.at[pl.ds(0, GX - 1)])
    without_own(sent)
    sent(5, ab_recv.at[pl.ds(0, GX - 1)])
    sent(6, e_recv.at[pl.ds(0, GX - 1)])
    sent(7, abl_recv.at[pl.ds(0, GY - 1)])
    sent(8, f_recv.at[pl.ds(0, GX - 1)])
    sent(9, h_recv.at[pl.ds(0, GX - 1)])
    sent(10, i_recv.at[pl.ds(0, GY - 1)])
    sent(11, j_recv.at[pl.ds(0, GX - 1)])


def body(
    hidden70,
    attn_gain,
    final_gain,
    query_weight,
    keyvalue_weight,
    out_weight,
    key_cache,
    value_cache,
    lengths,
    head70,
    adjusted_hidden,
    adjusted_gain,
    adjusted_head,
    base_hidden,
    base_gain,
    base_head,
):
    vocab = head70.shape[1]
    operands = (
        hidden70,
        attn_gain.reshape(1, -1),
        final_gain.reshape(1, -1),
        query_weight,
        keyvalue_weight.T,
        out_weight,
        key_cache,
        value_cache,
        head70.T,
        adjusted_hidden,
        adjusted_gain.reshape(1, -1),
        adjusted_head.T,
        base_hidden,
        base_gain.reshape(1, -1),
        base_head.T,
    )

    def like(a):
        return pltpu.VMEM(a.shape, a.dtype)

    caches = pltpu.VMEM((2, *key_cache.shape), BF)
    local = [like(a) for a in operands[:6]] + [caches] + [like(a) for a in operands[8:]]
    exchange = [
        pltpu.VMEM((4, 128), BF),
        pltpu.VMEM((GX, 4, 128), BF),
        pltpu.VMEM((2, 128), F32),
        pltpu.VMEM((GY, 2, 128), F32),
        pltpu.VMEM((GX, 2, 8, 128), BF),
        pltpu.VMEM((4, 128), BF),
        pltpu.VMEM((GX, 4, 128), BF),
        pltpu.VMEM((GX, 4, 128), BF),
        pltpu.VMEM((GX, 4, 128), BF),
        pltpu.VMEM((GX, 1, 128), F32),
        pltpu.VMEM((4 * GY, 1, 128), F32),
        pltpu.VMEM((2, 2, 128), BF),
        pltpu.VMEM((GX, 2, 128), BF),
        pltpu.VMEM((GX, 4, 128), BF),
        pltpu.VMEM((GX, 4, 128), BF),
        pltpu.VMEM((4, 128), BF),
        pltpu.VMEM((GX, 4, 128), BF),
        pltpu.VMEM((GY, 2, vocab), F32),
        pltpu.VMEM((GY, 2, vocab), F32),
        pltpu.VMEM((GY, 2, 1024 + 128), F32),
        pltpu.VMEM((GY, 2, 1024 + 128), F32),
        pltpu.VMEM((2, 128), F32),
        pltpu.VMEM((GX, 2, 128), F32),
    ]
    return pl.pallas_call(
        kernel,
        out_shape=jax.ShapeDtypeStruct((2, vocab), F32),
        in_specs=[pl.BlockSpec(memory_space=pltpu.SMEM)]
        + [pl.BlockSpec(memory_space=pl.ANY)] * len(operands),
        out_specs=pl.BlockSpec(memory_space=pltpu.VMEM),
        scratch_shapes=local
        + exchange
        + [
            pltpu.SemaphoreType.DMA((17,)),
            pltpu.SemaphoreType.DMA((12,)),
            pltpu.SemaphoreType.DMA((12,)),
            pltpu.SemaphoreType.REGULAR,
        ],
        compiler_params=pltpu.CompilerParams(collective_id=0, has_side_effects=True),
    )(lengths, *operands)


def solution(mesh):
    placed = (
        P("gx", "gy"),
        P("gy"),
        P("gy"),
        P("gy", "gx"),
        P("gy", "gx"),
        P("gx", "gy"),
        P("gy", "gx", None),
        P("gy", "gx", None),
        P("gy"),
        P("gy", "gx"),
        P("gx", "gy"),
        P("gy"),
        P("gy", "gx"),
        P("gx", "gy"),
        P("gy"),
        P("gy", "gx"),
    )
    return jax.shard_map(body, mesh=mesh, in_specs=placed, out_specs=P("gy", "gx"), check_vma=False)
```

```python
import functools
import math

import jax
import jax.numpy as jnp
from jax import lax
from jax.experimental import pallas as pl
from jax.experimental.pallas import tpu as pltpu
from jax.sharding import PartitionSpec as P

D = 8192
HEADS = 64
KV_HEADS = 8
HEAD_DIM = 128
D7 = 4096
CTX = 256

EPS = 1e-05
THETA = 10000.0
NEGATIVE = -1e30

GX = 32
GY = 16
NZ = 8
WIDTH = 1024
MESH = pl.DeviceIdType.MESH
BF = jnp.bfloat16
F32 = jnp.float32


def times_transposed(a, b):
    return lax.dot_general(a, b, (((1,), (1,)), ((), ())), preferred_element_type=F32)


def kernel(
    lengths,
    hidden,
    attn_gain,
    final_gain,
    query_weight,
    keyvalue_weight,
    out_weight,
    key_cache,
    value_cache,
    head70,
    adjusted_hidden,
    adjusted_gain,
    adjusted_head,
    base_hidden,
    base_gain,
    base_head,
    out,
    hid_v,
    ag_v,
    fg_v,
    qw_v,
    kvw_v,
    ow_v,
    kv_v,
    h70_v,
    ah_v,
    agn_v,
    ahead_v,
    bh_v,
    bgn_v,
    bhead_v,
    lens_v,
    x_send,
    x_recv,
    st_send,
    st_recv,
    kvw_recv,
    rows_recv,
    cache_recv,
    ab_send,
    ab_recv,
    q_send,
    q_recv,
    kn_send,
    kn_recv,
    e_send,
    e_recv,
    f_send,
    f_recv,
    h_send,
    h_recv,
    abl_send,
    abl_recv,
    i_send,
    i_recv,
    j_send,
    j_recv,
    load_sem,
    send_sem,
    recv_sem,
):
    gx = lax.axis_index("gx")
    gy = lax.axis_index("gy")
    z = gx // 4
    yh = (gx // 2) % 2
    core = gx % 2
    group = gx % 4
    pair = gx - core
    row = 2 * gy + core

    y_lo, x = gy // 4, gy % 4
    plane_y = (3 - y_lo, lax.rem(y_lo + 2, 4), y_lo + 1 - 2 * (y_lo % 2), y_lo)
    plane_x = (lax.rem(x + 2, 4), lax.rem(x + 1, 4), lax.rem(x + 3, 4), x)
    others = [4 * b + a for b in plane_y for a in plane_x][:-1]
    far_z = [lax.rem(z + k, NZ) for k in (4, 3, 5, 2, 6, 1, 7)]

    others_of_group = [lax.rem(group + k, 4) for k in (2, 3, 1)]

    def signal(to):
        pl.semaphore_signal(barrier, inc=1, device_id=to, device_id_type=MESH)

    def over(count, act, first=1):
        lax.fori_loop(first, count, lambda k, c: (act(k), c)[1], 0)

    head_to = (2 * z + yh) % NZ
    block_to = 4 * head_to + 2 * yh + z // 4
    keeps_block = block_to == gx
    projects = yh == z % 2

    pairs = [
        (hidden, hid_v),
        (adjusted_hidden, ah_v),
        (base_hidden, bh_v),
        (adjusted_gain, agn_v),
        (base_gain, bgn_v),
        (attn_gain, ag_v),
        (key_cache, kv_v.at[0]),
        (value_cache, kv_v.at[1]),
        (query_weight, qw_v),
        (keyvalue_weight, kvw_v),
        (out_weight, ow_v),
        (adjusted_head, ahead_v),
        (base_head, bhead_v),
        (final_gain, fg_v),
        (head70, h70_v),
    ]
    loads = [
        pltpu.make_async_copy(src, dst, load_sem.at[n]) for n, (src, dst) in enumerate(pairs)
    ]
    lens_load = pltpu.make_async_copy(lengths, lens_v, load_sem.at[len(pairs) + 2])
    loads[0].start()
    own_cache = [
        pltpu.make_async_copy(
            src.at[:, :, pl.ds(pl.multiple_of(z * HEAD_DIM, HEAD_DIM), HEAD_DIM)],
            rows_recv.at[z, n],
            load_sem.at[len(pairs) + n],
        )
        for n, src in enumerate((key_cache, value_cache))
    ]

    barrier = pltpu.get_barrier_semaphore()
    for g in others_of_group:
        signal((4 * z + g, gy))
    for t in far_z:
        signal((gx + 4 * (t - z), gy))
    for t in others:
        signal((gx, t))
    for half_block in range(2):
        source = 4 * (core * 4 + z // 2) + 2 * yh + half_block

        @pl.when(jnp.logical_and(projects, source != gx))
        def _(source=source):
            signal((source, gy))

    for load in [loads[6], loads[7], loads[9], *own_cache, *loads[1:6], loads[8], lens_load, *loads[10:]]:
        load.start()

    def send(n, src, dst, to):
        pltpu.make_async_remote_copy(
            src_ref=src,
            dst_ref=dst,
            send_sem=send_sem.at[n],
            recv_sem=recv_sem.at[n],
            device_id=to,
            device_id_type=MESH,
        ).start()

    def arrived(n, ref):
        pltpu.make_async_copy(ref, ref, recv_sem.at[n]).wait()

    def sent(n, ref):
        pltpu.make_async_copy(ref, ref, send_sem.at[n]).wait()

    def as_tiles(x, width):
        return [x[:, n * 128 : (n + 1) * 128] for n in range(width // 128)]

    def from_tiles(x):
        return jnp.concatenate([x[:, n, :] for n in range(4)], axis=1)

    loads[0].wait()
    x_send[...] = jnp.concatenate(as_tiles(hid_v[...].astype(F32), 512), axis=0).astype(BF)
    x_recv[z, yh, core] = x_send[...]
    loads[1].wait()
    loads[2].wait()
    adjusted_in = ah_v[...].astype(F32)
    base_in = bh_v[...].astype(F32)
    sum_adjusted = jnp.sum(adjusted_in * adjusted_in, axis=1, keepdims=True)
    sum_base = jnp.sum(base_in * base_in, axis=1, keepdims=True)
    st_send[...] = jnp.concatenate(
        [jnp.broadcast_to(sum_adjusted, (1, 128)), jnp.broadcast_to(sum_base, (1, 128))], axis=0
    )
    st_recv[gy] = st_send[...]
    greeted = NZ - 1 + 3 + GY - 1

    @pl.when(keeps_block)
    def _():
        pl.semaphore_wait(barrier, greeted)

    @pl.when(jnp.logical_not(keeps_block))
    def _():
        pl.semaphore_wait(barrier, greeted + 1)

    def over_group(act):
        for g in others_of_group:
            act(g)

    def over_z(act):
        for t in far_z:
            act(t)

    def head_of(t):
        return pl.ds(pl.multiple_of(t * HEAD_DIM, HEAD_DIM), HEAD_DIM)

    three_tiles = ab_recv.at[pl.ds(0, 3)]
    three_rows = cache_recv.reshape(NZ, 4, 2, 8, HEAD_DIM).at[:, pl.ds(0, 3)]

    over_group(lambda g: send(0, x_send, x_recv.at[z, yh, core], (4 * z + g, gy)))
    loads[9].wait()

    @pl.when(keeps_block)
    def _():
        kvw_recv[core] = kvw_v[...]

    @pl.when(jnp.logical_not(keeps_block))
    def _():
        send(12, kvw_v, kvw_recv.at[core], (block_to, gy))

    loads[6].wait()
    loads[7].wait()
    over_z(
        lambda t: send(2, kv_v.at[:, :, :, head_of(t)], rows_recv.at[z], (gx + 4 * (t - z), gy))
    )
    for t in others:
        send(1, st_send, st_recv.at[gy], (gx, t))
    arrived(0, three_tiles)

    over_z(lambda t: send(13, x_recv.at[z], x_recv.at[z], (gx + 4 * (t - z), gy)))

    def over_gx(act):
        for flip in (1, 0):
            side = 2 * (yh * (1 - flip) + (1 - yh) * flip)
            for to in far_z:
                for c in range(2):
                    act((4 * to + side + c, gy))
        for c in range(2):
            act((4 * z + 2 - 2 * yh + c, gy))
        act((pair + 1 - core, gy))

    arrived(1, st_recv.at[pl.ds(0, GY - 1)])
    totals = jnp.sum(st_recv[...], axis=0)
    loads[3].wait()
    loads[4].wait()
    adjusted = adjusted_in * lax.rsqrt(totals[0:1, 0:1] / D7 + EPS) * agn_v[...]
    base = base_in * lax.rsqrt(totals[1:2, 0:1] / D7 + EPS) * bgn_v[...]
    ab_send[...] = jnp.concatenate(as_tiles(adjusted, 256) + as_tiles(base, 256), axis=0).astype(BF)
    ab_recv[gx] = ab_send[...]
    over_gx(lambda to: send(5, ab_send, ab_recv.at[gx], to))

    for load in own_cache:
        load.wait()
    arrived(2, rows_recv.at[pl.ds(0, NZ - 1)])
    over_group(
        lambda g: send(
            16,
            rows_recv.at[:, :, lax.rem(g, 2)],
            cache_recv.at[:, yh, core],
            (4 * z + g, gy),
        )
    )
    cache_recv[:, yh, core] = rows_recv[:, :, core]

    lane = lax.broadcasted_iota(jnp.int32, (1, HEAD_DIM), 1)
    half = HEAD_DIM // 2
    turn = (lane % half).astype(F32)
    freq = jnp.exp(turn * (-2.0 / HEAD_DIM * math.log(THETA)))
    lens_load.wait()
    length = lens_v[core]
    angle = length.astype(F32) * freq
    cosine = jnp.cos(angle)
    sine = jnp.where(lane < half, -jnp.sin(angle), jnp.sin(angle))

    loads[5].wait()
    loads[8].wait()

    arrived(13, x_recv.at[pl.ds(0, NZ - 1)])
    rows = from_tiles(x_recv[...].astype(F32).reshape(GX, 4, 128))
    squares = jnp.sum(rows * rows, axis=1, keepdims=True)
    scaled = (rows * ag_v[...]).astype(BF)

    @pl.when(projects)
    def _():
        @pl.when(keeps_block)
        def _():
            arrived(12, kvw_recv.at[0])

        @pl.when(jnp.logical_not(keeps_block))
        def _():
            arrived(12, kvw_recv)

        weight = kvw_recv[...].reshape(HEAD_DIM, 512)
        kn_send[...] = times_transposed(scaled, weight).reshape(GX, 1, 128)
        kn_recv[core, gy] = kn_send[row]

        for g in [4 * b + a for b in plane_y[::-1] for a in plane_x]:
            for c in range(2):
                send(15, kn_send.at[2 * g + c], kn_recv.at[core, gy], (4 * z + 2 - 2 * yh + c, g))

    part_q = jnp.dot(scaled, qw_v[...], preferred_element_type=F32)
    high = squares.astype(BF).astype(F32)
    low = squares - high
    pieces = [
        part_q[:, :128],
        part_q[:, 128:],
        jnp.broadcast_to(high, (GX, 128)),
        jnp.broadcast_to(low, (GX, 128)),
    ]
    q_send[...] = jnp.concatenate([p.reshape(GX, 1, 128) for p in pieces], axis=1).astype(BF)
    q_recv[row] = q_send[row]

    def over_plane(act):
        for g in others:
            for c in range(2):
                act(c, 2 * g + c, (pair + c, g))
        act(1 - core, 2 * gy + 1 - core, (pair + 1 - core, gy))

    over_plane(lambda c, r, to: send(3, q_send.at[r], q_recv.at[row], to))

    @pl.when(projects)
    def _():
        over_plane(lambda c, r, to: send(4, kn_send.at[r], kn_recv.at[core, gy], to))

    arrived(5, ab_recv.at[pl.ds(0, GX - 1)])
    joined = from_tiles(ab_recv[...].astype(F32)).astype(BF)
    loads[11].wait()
    loads[12].wait()
    part_ab = times_transposed(joined[:, :256], ahead_v[...]) - times_transposed(
        joined[:, 256:], bhead_v[...]
    )
    vocab = part_ab.shape[1]
    for n in range(GY):
        abl_send[n] = part_ab[2 * n : 2 * n + 2]
    abl_recv[gy] = abl_send[gy]

    arrived(16, three_rows)
    cached = cache_recv[...].reshape(GX, 2, 8, HEAD_DIM).astype(F32)
    keys = cached[:, 0].reshape(CTX, HEAD_DIM).astype(BF)
    values = cached[:, 1].reshape(CTX, HEAD_DIM).astype(BF)

    arrived(3, q_recv.at[pl.ds(0, GX - 1)])
    q_total = jnp.zeros((2, 4, 128), F32)
    for n in range(GY):
        q_total = q_total + q_recv[2 * n : 2 * n + 2].astype(F32)
    square = q_total[0, 2:3, :] + q_total[0, 3:4, :]
    factor = lax.rsqrt(square / D + EPS)
    query = jnp.concatenate([q_total[0, 0:2, :], q_total[1, 0:2, :]], axis=0) * factor
    query = query.astype(BF).astype(F32)
    scale = HEAD_DIM ** (-0.5)
    turned = (query * cosine + pltpu.roll(query, half, 1) * sine).astype(BF)
    scores = times_transposed(turned, keys) * scale
    position = lax.broadcasted_iota(jnp.int32, (4, CTX), 1)
    valid = position < length
    scores = jnp.where(valid, scores, NEGATIVE)
    top = jnp.max(scores, axis=1, keepdims=True)

    @pl.when(projects)
    def _():
        arrived(4, kn_recv.reshape(2 * GY, 1, 128).at[pl.ds(0, 2 * GY - 1)])

    @pl.when(jnp.logical_not(projects))
    def _():
        arrived(15, kn_recv)

    fresh_kv = jnp.sum(kn_recv[...], axis=1)
    key_new = (fresh_kv[0] * factor).astype(BF).astype(F32)
    value_new = (fresh_kv[1] * factor).astype(BF).astype(F32)
    fresh_score = jnp.sum(query * key_new, axis=1, keepdims=True) * scale
    top = jnp.maximum(top, fresh_score)
    weights = jnp.where(valid, jnp.exp(scores - top), 0.0)
    fresh = jnp.exp(fresh_score - top)
    total = jnp.sum(weights, axis=1, keepdims=True) + fresh
    summed = jnp.dot(weights.astype(BF), values, preferred_element_type=F32)
    summed = summed + fresh.astype(BF).astype(F32) * value_new
    attn = (summed / total).astype(BF)
    e_send[0] = attn[0:2]
    e_send[1] = attn[2:4]
    e_recv[row] = e_send[core]

    over_plane(lambda c, r, to: send(6, e_send.at[c], e_recv.at[row], to))

    def to_gy(n, src, dst):
        for t in others:
            send(n, src.at[t], dst.at[gy], (gx, t))

    to_gy(7, abl_send, abl_recv)

    loads[10].wait()
    arrived(6, e_recv.at[pl.ds(0, GX - 1)])
    heads = e_recv[...].astype(F32)
    heads = jnp.concatenate([heads[:, 0, :], heads[:, 1, :]], axis=1).astype(BF)
    mixed = jnp.dot(heads, ow_v[...], preferred_element_type=F32)
    tiles = jnp.concatenate([p.reshape(GX, 1, 128) for p in as_tiles(mixed, 512)], axis=1)
    f_send[...] = tiles.astype(BF).reshape(NZ, 2, 2, 4, 128)
    slot = 2 * z + core
    f_recv[slot] = f_send[z, :, core]

    def over_half(act):
        for to in far_z:
            for c in range(2):
                act(to, c, (4 * to + 2 * yh + c, gy))
        act(z, 1 - core, (pair + 1 - core, gy))

    over_half(lambda d, c, to: send(8, f_send.at[d, :, c], f_recv.at[slot], to))
    arrived(7, abl_recv.at[pl.ds(0, GY - 1)])
    ab_logits = jnp.sum(abl_recv[...], axis=0)
    loads[13].wait()
    loads[14].wait()
    own_rows = x_recv[z, :, core].astype(F32)
    arrived(8, f_recv.at[pl.ds(0, 15)])
    partial = jnp.sum(f_recv[...].astype(F32), axis=0)

    h_send[...] = (partial + own_rows * jnp.where(yh == 0, 1.0, 0.0)).astype(BF)
    h_recv[yh, z, :, core] = h_send[...]
    over_gx(lambda to: send(9, h_send, h_recv.at[yh, z, :, core], to))
    arrived(9, h_recv.reshape(GX, 2, 4, 128).at[pl.ds(0, GX - 1)])
    halves = h_recv[...].astype(F32)
    rows = from_tiles((halves[0] + halves[1]).reshape(GX, 4, 128))
    squares = jnp.sum(rows * rows, axis=1, keepdims=True)
    scaled = (rows * fg_v[...]).astype(BF)
    part = times_transposed(scaled, h70_v[...])
    high = squares.astype(BF).astype(F32)
    low = squares - high
    rest = (WIDTH - vocab) // 2
    tail = [jnp.broadcast_to(high, (GX, rest)), jnp.broadcast_to(low, (GX, rest))]
    part = jnp.concatenate([part, *tail], axis=1).astype(BF)
    for n in range(GY):
        i_send[n] = part[2 * n : 2 * n + 2]
    i_recv[gy] = i_send[gy]

    to_gy(10, i_send, i_recv)
    arrived(10, i_recv.at[pl.ds(0, GY - 1)])
    summed = jnp.sum(i_recv[...].astype(F32), axis=0)
    square = summed[:, vocab : vocab + 1] + summed[:, WIDTH - 1 :]
    factor = lax.rsqrt(square / D + EPS)
    logits = summed[:, :vocab] * factor + ab_logits
    peak = jnp.max(logits, axis=1, keepdims=True)
    partial_lse = peak + jnp.log(jnp.sum(jnp.exp(logits - peak), axis=1, keepdims=True))
    j_send[...] = jnp.broadcast_to(partial_lse, (2, 128))
    j_recv[gx] = j_send[...]

    over_gx(lambda to: send(11, j_send, j_recv.at[gx], to))
    arrived(11, j_recv.at[pl.ds(0, GX - 1)])
    everyone = j_recv[...]
    peak = jnp.max(everyone, axis=0)
    lse = peak + jnp.log(jnp.sum(jnp.exp(everyone - peak[None]), axis=0))
    out[...] = logits - lse[:, 0:1]

    sent(0, three_tiles)
    sent(1, st_recv.at[pl.ds(0, GY - 1)])
    sent(2, rows_recv.at[pl.ds(0, NZ - 1)])
    sent(3, q_recv.at[pl.ds(0, GX - 1)])

    @pl.when(projects)
    def _():
        sent(15, kn_send)
        sent(4, kn_send.at[pl.ds(0, GX - 1)])

    sent(5, ab_recv.at[pl.ds(0, GX - 1)])
    sent(6, e_recv.at[pl.ds(0, GX - 1)])
    sent(7, abl_recv.at[pl.ds(0, GY - 1)])
    sent(8, f_recv.at[pl.ds(0, 15)])
    sent(9, h_recv.reshape(GX, 2, 4, 128).at[pl.ds(0, GX - 1)])
    sent(10, i_recv.at[pl.ds(0, GY - 1)])
    sent(11, j_recv.at[pl.ds(0, GX - 1)])

    @pl.when(jnp.logical_not(keeps_block))
    def _():
        sent(12, kvw_v)

    sent(13, x_recv.at[pl.ds(0, NZ - 1)])
    sent(16, three_rows)


def body(
    hidden70,
    attn_gain,
    final_gain,
    query_weight,
    keyvalue_weight,
    out_weight,
    key_cache,
    value_cache,
    lengths,
    head70,
    adjusted_hidden,
    adjusted_gain,
    adjusted_head,
    base_hidden,
    base_gain,
    base_head,
):
    vocab = head70.shape[1]
    operands = (
        hidden70,
        attn_gain.reshape(1, -1),
        final_gain.reshape(1, -1),
        query_weight,
        keyvalue_weight.T,
        out_weight,
        key_cache,
        value_cache,
        head70.T,
        adjusted_hidden,
        adjusted_gain.reshape(1, -1),
        adjusted_head.T,
        base_hidden,
        base_gain.reshape(1, -1),
        base_head.T,
    )

    def like(a):
        return pltpu.VMEM(a.shape, a.dtype)

    caches = pltpu.VMEM((2, *key_cache.shape), BF)
    local = [like(a) for a in operands[:6]] + [caches] + [like(a) for a in operands[8:]]
    vm = pltpu.VMEM
    exchange = [
        vm((4, 128), BF),
        vm((NZ, 2, 2, 4, 128), BF),
        vm((2, 128), F32),
        vm((GY, 2, 128), F32),
        vm((2, 64, 512), BF),
        vm((NZ, 2, 2, 8, HEAD_DIM), BF),
        vm((NZ, 2, 2, 2, 8, 128), BF),
        vm((4, 128), BF),
        vm((GX, 4, 128), BF),
        vm((GX, 4, 128), BF),
        vm((GX, 4, 128), BF),
        vm((GX, 1, 128), F32),
        vm((2, GY, 1, 128), F32),
        vm((2, 2, 128), BF),
        vm((GX, 2, 128), BF),
        vm((NZ, 2, 2, 4, 128), BF),
        vm((16, 2, 4, 128), BF),
        vm((2, 4, 128), BF),
        vm((2, NZ, 2, 2, 4, 128), BF),
        vm((GY, 2, vocab), F32),
        vm((GY, 2, vocab), F32),
        vm((GY, 2, WIDTH), BF),
        vm((GY, 2, WIDTH), BF),
        vm((2, 128), F32),
        vm((GX, 2, 128), F32),
    ]
    return pl.pallas_call(
        kernel,
        out_shape=pltpu.VMEM((2, vocab), F32),
        in_specs=[pl.BlockSpec(memory_space=pl.ANY)] * (1 + len(operands)),
        out_specs=pl.BlockSpec(memory_space=pltpu.VMEM),
        scratch_shapes=local
        + [pltpu.SMEM(lengths.shape, lengths.dtype)]
        + exchange
        + [
            pltpu.SemaphoreType.DMA((18,)),
            pltpu.SemaphoreType.DMA((17,)),
            pltpu.SemaphoreType.DMA((17,)),
        ],
        compiler_params=pltpu.CompilerParams(collective_id=0, has_side_effects=True),
    )(lengths, *operands)


def solution(mesh):
    placed = (
        P("gx", "gy"),
        P("gy"),
        P("gy"),
        P("gy", "gx"),
        P("gy", "gx"),
        P("gx", "gy"),
        P("gy", "gx", None),
        P("gy", "gx", None),
        P("gy"),
        P("gy", "gx"),
        P("gx", "gy"),
        P("gy"),
        P("gy", "gx"),
        P("gx", "gy"),
        P("gy"),
        P("gy", "gx"),
    )
    return jax.shard_map(body, mesh=mesh, in_specs=placed, out_specs=P("gy", "gx"), check_vma=False)
```

```python
import functools
import math

import jax
import jax.numpy as jnp
from jax import lax
from jax.experimental import pallas as pl
from jax.experimental.pallas import tpu as pltpu
from jax.sharding import PartitionSpec as P

D = 8192
HEADS = 64
KV_HEADS = 8
HEAD_DIM = 128
D7 = 4096
CTX = 256

EPS = 1e-05
THETA = 10000.0
NEGATIVE = -1e30

GX = 32
GY = 16
NZ = 8
WIDTH = 1024
MESH = pl.DeviceIdType.MESH
BF = jnp.bfloat16
F32 = jnp.float32


def times_transposed(a, b):
    return lax.dot_general(a, b, (((1,), (1,)), ((), ())), preferred_element_type=F32)


def kernel(
    lengths,
    hidden,
    attn_gain,
    final_gain,
    query_weight,
    keyvalue_weight,
    out_weight,
    key_cache,
    value_cache,
    head70,
    adjusted_hidden,
    adjusted_gain,
    adjusted_head,
    base_hidden,
    base_gain,
    base_head,
    out,
    hid_v,
    ag_v,
    fg_v,
    qw_v,
    kvw_v,
    ow_v,
    kv_v,
    h70_v,
    ah_v,
    agn_v,
    ahead_v,
    bh_v,
    bgn_v,
    bhead_v,
    lens_v,
    x_send,
    x_recv,
    st_send,
    st_recv,
    kvw_recv,
    rows_recv,
    cache_recv,
    ab_send,
    ab_recv,
    q_send,
    q_recv,
    kn_send,
    kn_recv,
    e_send,
    e_recv,
    f_send,
    f_recv,
    h_send,
    h_recv,
    abl_send,
    abl_recv,
    i_send,
    i_recv,
    j_send,
    j_recv,
    load_sem,
    send_sem,
    recv_sem,
):
    gx = lax.axis_index("gx")
    gy = lax.axis_index("gy")
    z = gx // 4
    yh = (gx // 2) % 2
    core = gx % 2
    group = gx % 4
    pair = gx - core
    row = 2 * gy + core

    y_lo, x = gy // 4, gy % 4
    plane_y = (3 - y_lo, lax.rem(y_lo + 2, 4), y_lo + 1 - 2 * (y_lo % 2), y_lo)
    plane_x = (lax.rem(x + 2, 4), lax.rem(x + 1, 4), lax.rem(x + 3, 4), x)
    others = [4 * b + a for b in plane_y for a in plane_x][:-1]
    far_z = [lax.rem(z + k, NZ) for k in (4, 3, 5, 2, 6, 1, 7)]

    others_of_group = [lax.rem(group + k, 4) for k in (2, 3, 1)]

    def signal(to):
        pl.semaphore_signal(barrier, inc=1, device_id=to, device_id_type=MESH)

    def over(count, act, first=1):
        lax.fori_loop(first, count, lambda k, c: (act(k), c)[1], 0)

    head_to = (2 * z + yh) % NZ
    block_to = 4 * head_to + 2 * yh + z // 4
    keeps_block = block_to == gx
    projects = yh == z % 2

    pairs = [
        (hidden, hid_v),
        (adjusted_hidden, ah_v),
        (base_hidden, bh_v),
        (adjusted_gain, agn_v),
        (base_gain, bgn_v),
        (attn_gain, ag_v),
        (key_cache, kv_v.at[0]),
        (value_cache, kv_v.at[1]),
        (query_weight, qw_v),
        (keyvalue_weight, kvw_v),
        (out_weight, ow_v),
        (adjusted_head, ahead_v),
        (base_head, bhead_v),
        (final_gain, fg_v),
        (head70, h70_v),
    ]
    loads = [
        pltpu.make_async_copy(src, dst, load_sem.at[n]) for n, (src, dst) in enumerate(pairs)
    ]
    lens_load = pltpu.make_async_copy(lengths, lens_v, load_sem.at[len(pairs) + 2])
    loads[0].start()
    own_cache = [
        pltpu.make_async_copy(
            src.at[:, :, pl.ds(pl.multiple_of(z * HEAD_DIM, HEAD_DIM), HEAD_DIM)],
            rows_recv.at[z, n],
            load_sem.at[len(pairs) + n],
        )
        for n, src in enumerate((key_cache, value_cache))
    ]

    barrier = pltpu.get_barrier_semaphore()
    for g in others_of_group:
        signal((4 * z + g, gy))
    for t in far_z:
        signal((gx + 4 * (t - z), gy))
    for t in others:
        signal((gx, t))
    for half_block in range(2):
        source = 4 * (core * 4 + z // 2) + 2 * yh + half_block

        @pl.when(jnp.logical_and(projects, source != gx))
        def _(source=source):
            signal((source, gy))

    for load in [loads[6], loads[7], loads[9], *own_cache, *loads[1:6], loads[8], lens_load, *loads[10:]]:
        load.start()

    def send(n, src, dst, to):
        pltpu.make_async_remote_copy(
            src_ref=src,
            dst_ref=dst,
            send_sem=send_sem.at[n],
            recv_sem=recv_sem.at[n],
            device_id=to,
            device_id_type=MESH,
        ).start()

    def arrived(n, ref):
        pltpu.make_async_copy(ref, ref, recv_sem.at[n]).wait()

    def sent(n, ref):
        pltpu.make_async_copy(ref, ref, send_sem.at[n]).wait()

    def as_tiles(x, width):
        return [x[:, n * 128 : (n + 1) * 128] for n in range(width // 128)]

    def from_tiles(x):
        return jnp.concatenate([x[:, n, :] for n in range(4)], axis=1)

    loads[0].wait()
    x_send[...] = jnp.concatenate(as_tiles(hid_v[...].astype(F32), 512), axis=0).astype(BF)
    x_recv[z, yh, core] = x_send[...]
    loads[1].wait()
    loads[2].wait()
    adjusted_in = ah_v[...].astype(F32)
    base_in = bh_v[...].astype(F32)
    sum_adjusted = jnp.sum(adjusted_in * adjusted_in, axis=1, keepdims=True)
    sum_base = jnp.sum(base_in * base_in, axis=1, keepdims=True)
    hidden_in = hid_v[...].astype(F32)
    sum_hidden = jnp.sum(hidden_in * hidden_in, axis=1, keepdims=True)
    sums = (sum_adjusted, sum_base, sum_hidden, sum_hidden)
    st_send[...] = jnp.concatenate([jnp.broadcast_to(t, (1, 128)) for t in sums], axis=0)
    st_recv[gy] = st_send[...]
    greeted = NZ - 1 + 3 + GY - 1

    @pl.when(keeps_block)
    def _():
        pl.semaphore_wait(barrier, greeted)

    @pl.when(jnp.logical_not(keeps_block))
    def _():
        pl.semaphore_wait(barrier, greeted + 1)

    def over_group(act):
        for g in others_of_group:
            act(g)

    def over_z(act):
        for t in far_z:
            act(t)

    def head_of(t):
        return pl.ds(pl.multiple_of(t * HEAD_DIM, HEAD_DIM), HEAD_DIM)

    three_tiles = x_recv.reshape(GX, 4, 128).at[pl.ds(0, 3)]
    three_rows = cache_recv.reshape(NZ, 4, 2, 8, HEAD_DIM).at[:, pl.ds(0, 3)]

    over_group(lambda g: send(0, x_send, x_recv.at[z, yh, core], (4 * z + g, gy)))
    loads[6].wait()
    loads[7].wait()
    over_z(
        lambda t: send(2, kv_v.at[:, :, :, head_of(t)], rows_recv.at[z], (gx + 4 * (t - z), gy))
    )
    loads[9].wait()

    @pl.when(keeps_block)
    def _():
        kvw_recv[core] = kvw_v[...]

    @pl.when(jnp.logical_not(keeps_block))
    def _():
        send(12, kvw_v, kvw_recv.at[core], (block_to, gy))

    for t in others:
        send(1, st_send, st_recv.at[gy], (gx, t))
    arrived(0, three_tiles)

    over_z(lambda t: send(13, x_recv.at[z], x_recv.at[z], (gx + 4 * (t - z), gy)))

    def over_gx(act):
        for flip in (1, 0):
            side = 2 * (yh * (1 - flip) + (1 - yh) * flip)
            for to in far_z:
                for c in range(2):
                    act((4 * to + side + c, gy))
        for c in range(2):
            act((4 * z + 2 - 2 * yh + c, gy))
        act((pair + 1 - core, gy))

    arrived(1, st_recv.at[pl.ds(0, GY - 1)])
    totals = jnp.sum(st_recv[...], axis=0)
    loads[3].wait()
    loads[4].wait()
    adjusted = adjusted_in * lax.rsqrt(totals[0:1, 0:1] / D7 + EPS) * agn_v[...]
    base = base_in * lax.rsqrt(totals[1:2, 0:1] / D7 + EPS) * bgn_v[...]
    factor = lax.rsqrt(totals[2:3, :] / D + EPS)
    high = factor.astype(BF).astype(F32)
    ab_send[...] = jnp.concatenate(
        as_tiles(adjusted, 256) + as_tiles(base, 256) + [high, factor - high], axis=0
    ).astype(BF)
    ab_recv[gx] = ab_send[...]
    over_gx(lambda to: send(5, ab_send, ab_recv.at[gx], to))

    for load in own_cache:
        load.wait()
    arrived(2, rows_recv.at[pl.ds(0, NZ - 1)])
    over_group(
        lambda g: send(
            16,
            rows_recv.at[:, :, lax.rem(g, 2)],
            cache_recv.at[:, yh, core],
            (4 * z + g, gy),
        )
    )
    cache_recv[:, yh, core] = rows_recv[:, :, core]

    lane = lax.broadcasted_iota(jnp.int32, (1, HEAD_DIM), 1)
    half = HEAD_DIM // 2
    turn = (lane % half).astype(F32)
    freq = jnp.exp(turn * (-2.0 / HEAD_DIM * math.log(THETA)))
    lens_load.wait()
    length = lens_v[core]
    angle = length.astype(F32) * freq
    cosine = jnp.cos(angle)
    sine = jnp.where(lane < half, -jnp.sin(angle), jnp.sin(angle))

    loads[5].wait()
    loads[8].wait()

    arrived(13, x_recv.at[pl.ds(0, NZ - 1)])
    rows = from_tiles(x_recv[...].astype(F32).reshape(GX, 4, 128))
    scaled = (rows * ag_v[...]).astype(BF)

    @pl.when(projects)
    def _():
        @pl.when(keeps_block)
        def _():
            arrived(12, kvw_recv.at[0])

        @pl.when(jnp.logical_not(keeps_block))
        def _():
            arrived(12, kvw_recv)

        weight = kvw_recv[...].reshape(HEAD_DIM, 512)
        kn_send[...] = times_transposed(scaled, weight).reshape(GX, 1, 128)
        kn_recv[core, gy] = kn_send[row]

        for g in [4 * b + a for b in plane_y[::-1] for a in plane_x]:
            for c in range(2):
                send(15, kn_send.at[2 * g + c], kn_recv.at[core, gy], (4 * z + 2 - 2 * yh + c, g))

    part_q = jnp.dot(scaled, qw_v[...], preferred_element_type=F32)
    q_send[...] = jnp.concatenate(
        [p.reshape(GX, 1, 128) for p in as_tiles(part_q, 256)], axis=1
    ).astype(BF)
    q_recv[row] = q_send[row]

    def over_plane(act):
        for g in others:
            for c in range(2):
                act(c, 2 * g + c, (pair + c, g))
        act(1 - core, 2 * gy + 1 - core, (pair + 1 - core, gy))

    over_plane(lambda c, r, to: send(3, q_send.at[r], q_recv.at[row], to))

    @pl.when(projects)
    def _():
        over_plane(lambda c, r, to: send(4, kn_send.at[r], kn_recv.at[core, gy], to))

    arrived(5, ab_recv.at[pl.ds(0, GX - 1)])
    joined = from_tiles(ab_recv[...].astype(F32)).astype(BF)
    loads[11].wait()
    loads[12].wait()
    part_ab = times_transposed(joined[:, :256], ahead_v[...]) - times_transposed(
        joined[:, 256:], bhead_v[...]
    )
    vocab = part_ab.shape[1]
    for n in range(GY):
        abl_send[n] = part_ab[2 * n : 2 * n + 2]
    abl_recv[gy] = abl_send[gy]
    parts = ab_recv[row].astype(F32)
    factor = parts[4:5, :] + parts[5:6, :]

    arrived(16, three_rows)
    cached = cache_recv[...].reshape(GX, 2, 8, HEAD_DIM).astype(F32)
    keys = cached[:, 0].reshape(CTX, HEAD_DIM).astype(BF)
    values = cached[:, 1].reshape(CTX, HEAD_DIM).astype(BF)

    arrived(3, q_recv.at[pl.ds(0, GX - 1)])
    q_total = jnp.zeros((2, 2, 128), F32)
    for n in range(GY):
        q_total = q_total + q_recv[2 * n : 2 * n + 2].astype(F32)
    query = jnp.concatenate([q_total[0], q_total[1]], axis=0) * factor
    query = query.astype(BF).astype(F32)
    scale = HEAD_DIM ** (-0.5)
    turned = (query * cosine + pltpu.roll(query, half, 1) * sine).astype(BF)
    scores = times_transposed(turned, keys) * scale
    position = lax.broadcasted_iota(jnp.int32, (4, CTX), 1)
    valid = position < length
    scores = jnp.where(valid, scores, NEGATIVE)
    top = jnp.max(scores, axis=1, keepdims=True)

    @pl.when(projects)
    def _():
        arrived(4, kn_recv.reshape(2 * GY, 1, 128).at[pl.ds(0, 2 * GY - 1)])

    @pl.when(jnp.logical_not(projects))
    def _():
        arrived(15, kn_recv)

    fresh_kv = jnp.sum(kn_recv[...], axis=1)
    key_new = (fresh_kv[0] * factor).astype(BF).astype(F32)
    value_new = (fresh_kv[1] * factor).astype(BF).astype(F32)
    fresh_score = jnp.sum(query * key_new, axis=1, keepdims=True) * scale
    top = jnp.maximum(top, fresh_score)
    weights = jnp.where(valid, jnp.exp(scores - top), 0.0)
    fresh = jnp.exp(fresh_score - top)
    total = jnp.sum(weights, axis=1, keepdims=True) + fresh
    summed = jnp.dot(weights.astype(BF), values, preferred_element_type=F32)
    summed = summed + fresh.astype(BF).astype(F32) * value_new
    attn = (summed / total).astype(BF)
    e_send[0] = attn[0:2]
    e_send[1] = attn[2:4]
    e_recv[row] = e_send[core]

    over_plane(lambda c, r, to: send(6, e_send.at[c], e_recv.at[row], to))

    def to_gy(n, src, dst):
        for t in others:
            send(n, src.at[t], dst.at[gy], (gx, t))


    loads[10].wait()
    arrived(6, e_recv.at[pl.ds(0, GX - 1)])
    heads = e_recv[...].astype(F32)
    heads = jnp.concatenate([heads[:, 0, :], heads[:, 1, :]], axis=1).astype(BF)
    mixed = jnp.dot(heads, ow_v[...], preferred_element_type=F32)
    tiles = jnp.concatenate([p.reshape(GX, 1, 128) for p in as_tiles(mixed, 512)], axis=1)
    f_send[...] = tiles.astype(BF).reshape(NZ, 2, 2, 4, 128)
    slot = 2 * z + core
    f_recv[slot] = f_send[z, :, core]

    def over_half(act):
        for to in far_z:
            for c in range(2):
                act(to, c, (4 * to + 2 * yh + c, gy))
        act(z, 1 - core, (pair + 1 - core, gy))

    over_half(lambda d, c, to: send(8, f_send.at[d, :, c], f_recv.at[slot], to))
    to_gy(7, abl_send, abl_recv)
    loads[13].wait()
    loads[14].wait()
    own_rows = x_recv[z, :, core].astype(F32)
    arrived(8, f_recv.at[pl.ds(0, 15)])
    partial = jnp.sum(f_recv[...].astype(F32), axis=0)

    h_send[...] = (partial + own_rows * jnp.where(yh == 0, 1.0, 0.0)).astype(BF)
    h_recv[yh, z, :, core] = h_send[...]
    over_gx(lambda to: send(9, h_send, h_recv.at[yh, z, :, core], to))
    arrived(7, abl_recv.at[pl.ds(0, GY - 1)])
    ab_logits = jnp.sum(abl_recv[...], axis=0)
    arrived(9, h_recv.reshape(GX, 2, 4, 128).at[pl.ds(0, GX - 1)])
    halves = h_recv[...].astype(F32)
    rows = from_tiles((halves[0] + halves[1]).reshape(GX, 4, 128))
    squares = jnp.sum(rows * rows, axis=1, keepdims=True)
    scaled = (rows * fg_v[...]).astype(BF)
    part = times_transposed(scaled, h70_v[...])
    high = squares.astype(BF).astype(F32)
    low = squares - high
    rest = (WIDTH - vocab) // 2
    tail = [jnp.broadcast_to(high, (GX, rest)), jnp.broadcast_to(low, (GX, rest))]
    part = jnp.concatenate([part, *tail], axis=1).astype(BF)
    for n in range(GY):
        i_send[n] = part[2 * n : 2 * n + 2]
    i_recv[gy] = i_send[gy]

    to_gy(10, i_send, i_recv)
    arrived(10, i_recv.at[pl.ds(0, GY - 1)])
    summed = jnp.sum(i_recv[...].astype(F32), axis=0)
    square = summed[:, vocab : vocab + 1] + summed[:, WIDTH - 1 :]
    factor = lax.rsqrt(square / D + EPS)
    logits = summed[:, :vocab] * factor + ab_logits
    peak = jnp.max(logits, axis=1, keepdims=True)
    partial_lse = peak + jnp.log(jnp.sum(jnp.exp(logits - peak), axis=1, keepdims=True))
    j_send[...] = jnp.broadcast_to(partial_lse, (2, 128))
    j_recv[gx] = j_send[...]

    over_gx(lambda to: send(11, j_send, j_recv.at[gx], to))
    arrived(11, j_recv.at[pl.ds(0, GX - 1)])
    everyone = j_recv[...]
    peak = jnp.max(everyone, axis=0)
    lse = peak + jnp.log(jnp.sum(jnp.exp(everyone - peak[None]), axis=0))
    out[...] = logits - lse[:, 0:1]

    sent(0, three_tiles)
    sent(1, st_recv.at[pl.ds(0, GY - 1)])
    sent(2, rows_recv.at[pl.ds(0, NZ - 1)])
    sent(3, q_recv.at[pl.ds(0, GX - 1)])

    @pl.when(projects)
    def _():
        sent(15, kn_send)
        sent(4, kn_send.at[pl.ds(0, GX - 1)])

    sent(5, ab_recv.at[pl.ds(0, GX - 1)])
    sent(6, e_recv.at[pl.ds(0, GX - 1)])
    sent(7, abl_recv.at[pl.ds(0, GY - 1)])
    sent(8, f_recv.at[pl.ds(0, 15)])
    sent(9, h_recv.reshape(GX, 2, 4, 128).at[pl.ds(0, GX - 1)])
    sent(10, i_recv.at[pl.ds(0, GY - 1)])
    sent(11, j_recv.at[pl.ds(0, GX - 1)])

    @pl.when(jnp.logical_not(keeps_block))
    def _():
        sent(12, kvw_v)

    sent(13, x_recv.at[pl.ds(0, NZ - 1)])
    sent(16, three_rows)


def body(
    hidden70,
    attn_gain,
    final_gain,
    query_weight,
    keyvalue_weight,
    out_weight,
    key_cache,
    value_cache,
    lengths,
    head70,
    adjusted_hidden,
    adjusted_gain,
    adjusted_head,
    base_hidden,
    base_gain,
    base_head,
):
    vocab = head70.shape[1]
    operands = (
        hidden70,
        attn_gain.reshape(1, -1),
        final_gain.reshape(1, -1),
        query_weight,
        keyvalue_weight.T,
        out_weight,
        key_cache,
        value_cache,
        head70.T,
        adjusted_hidden,
        adjusted_gain.reshape(1, -1),
        adjusted_head.T,
        base_hidden,
        base_gain.reshape(1, -1),
        base_head.T,
    )

    def like(a):
        return pltpu.VMEM(a.shape, a.dtype)

    caches = pltpu.VMEM((2, *key_cache.shape), BF)
    local = [like(a) for a in operands[:6]] + [caches] + [like(a) for a in operands[8:]]
    vm = pltpu.VMEM
    exchange = [
        vm((4, 128), BF),
        vm((NZ, 2, 2, 4, 128), BF),
        vm((4, 128), F32),
        vm((GY, 4, 128), F32),
        vm((2, 64, 512), BF),
        vm((NZ, 2, 2, 8, HEAD_DIM), BF),
        vm((NZ, 2, 2, 2, 8, 128), BF),
        vm((6, 128), BF),
        vm((GX, 6, 128), BF),
        vm((GX, 2, 128), BF),
        vm((GX, 2, 128), BF),
        vm((GX, 1, 128), F32),
        vm((2, GY, 1, 128), F32),
        vm((2, 2, 128), BF),
        vm((GX, 2, 128), BF),
        vm((NZ, 2, 2, 4, 128), BF),
        vm((16, 2, 4, 128), BF),
        vm((2, 4, 128), BF),
        vm((2, NZ, 2, 2, 4, 128), BF),
        vm((GY, 2, vocab), F32),
        vm((GY, 2, vocab), F32),
        vm((GY, 2, WIDTH), BF),
        vm((GY, 2, WIDTH), BF),
        vm((2, 128), F32),
        vm((GX, 2, 128), F32),
    ]
    return pl.pallas_call(
        kernel,
        out_shape=pltpu.VMEM((2, vocab), F32),
        in_specs=[pl.BlockSpec(memory_space=pl.ANY)] * (1 + len(operands)),
        out_specs=pl.BlockSpec(memory_space=pltpu.VMEM),
        scratch_shapes=local
        + [pltpu.SMEM(lengths.shape, lengths.dtype)]
        + exchange
        + [
            pltpu.SemaphoreType.DMA((18,)),
            pltpu.SemaphoreType.DMA((17,)),
            pltpu.SemaphoreType.DMA((17,)),
        ],
        compiler_params=pltpu.CompilerParams(collective_id=0, has_side_effects=True),
    )(lengths, *operands)


def solution(mesh):
    placed = (
        P("gx", "gy"),
        P("gy"),
        P("gy"),
        P("gy", "gx"),
        P("gy", "gx"),
        P("gx", "gy"),
        P("gy", "gx", None),
        P("gy", "gx", None),
        P("gy"),
        P("gy", "gx"),
        P("gx", "gy"),
        P("gy"),
        P("gy", "gx"),
        P("gx", "gy"),
        P("gy"),
        P("gy", "gx"),
    )
    return jax.shard_map(body, mesh=mesh, in_specs=placed, out_specs=P("gy", "gx"), check_vma=False)
```

```python
import functools
import math

import jax
import jax.numpy as jnp
from jax import lax
from jax.experimental import pallas as pl
from jax.experimental.pallas import tpu as pltpu
from jax.sharding import PartitionSpec as P

D = 8192
HEADS = 64
KV_HEADS = 8
HEAD_DIM = 128
D7 = 4096
CTX = 256

EPS = 1e-05
THETA = 10000.0
NEGATIVE = -1e30

GX = 32
GY = 16
NZ = 8
WIDTH = 1024
MESH = pl.DeviceIdType.MESH
BF = jnp.bfloat16
F32 = jnp.float32


def times_transposed(a, b):
    return lax.dot_general(a, b, (((1,), (1,)), ((), ())), preferred_element_type=F32)


def kernel(
    lengths,
    hidden,
    attn_gain,
    final_gain,
    query_weight,
    keyvalue_weight,
    out_weight,
    key_cache,
    value_cache,
    head70,
    adjusted_hidden,
    adjusted_gain,
    adjusted_head,
    base_hidden,
    base_gain,
    base_head,
    out,
    hid_v,
    ag_v,
    fg_v,
    qw_v,
    kvw_v,
    ow_v,
    kv_v,
    h70_v,
    ah_v,
    agn_v,
    ahead_v,
    bh_v,
    bgn_v,
    bhead_v,
    lens_v,
    x_send,
    x_recv,
    st_send,
    st_recv,
    kvw_recv,
    rows_recv,
    cache_recv,
    ab_send,
    ab_recv,
    q_send,
    q_recv,
    kn_send,
    kn_recv,
    e_send,
    e_recv,
    f_send,
    f_recv,
    h_send,
    h_recv,
    abl_send,
    abl_recv,
    i_send,
    i_recv,
    j_send,
    j_recv,
    load_sem,
    send_sem,
    recv_sem,
):
    gx = lax.axis_index("gx")
    gy = lax.axis_index("gy")
    z = gx // 4
    yh = (gx // 2) % 2
    core = gx % 2
    group = gx % 4
    pair = gx - core
    row = 2 * gy + core

    y_lo, x = gy // 4, gy % 4
    plane_y = (3 - y_lo, lax.rem(y_lo + 2, 4), y_lo + 1 - 2 * (y_lo % 2), y_lo)
    plane_x = (lax.rem(x + 2, 4), lax.rem(x + 1, 4), lax.rem(x + 3, 4), x)
    others = [4 * b + a for b in plane_y for a in plane_x][:-1]
    far_z = [lax.rem(z + k, NZ) for k in (4, 3, 5, 2, 6, 1, 7)]

    others_of_group = [lax.rem(group + k, 4) for k in (2, 3, 1)]

    def signal(to):
        pl.semaphore_signal(barrier, inc=1, device_id=to, device_id_type=MESH)

    def over(count, act, first=1):
        lax.fori_loop(first, count, lambda k, c: (act(k), c)[1], 0)

    head_to = (2 * z + yh) % NZ
    block_to = 4 * head_to + 2 * yh + z // 4
    keeps_block = block_to == gx
    projects = yh == z % 2

    pairs = [
        (hidden, hid_v),
        (adjusted_hidden, ah_v),
        (base_hidden, bh_v),
        (adjusted_gain, agn_v),
        (base_gain, bgn_v),
        (attn_gain, ag_v),
        (key_cache, kv_v.at[0]),
        (value_cache, kv_v.at[1]),
        (query_weight, qw_v),
        (keyvalue_weight, kvw_v),
        (out_weight, ow_v),
        (adjusted_head, ahead_v),
        (base_head, bhead_v),
        (final_gain, fg_v),
        (head70, h70_v),
    ]
    loads = [
        pltpu.make_async_copy(src, dst, load_sem.at[n]) for n, (src, dst) in enumerate(pairs)
    ]
    lens_load = pltpu.make_async_copy(lengths, lens_v, load_sem.at[len(pairs) + 2])
    loads[0].start()
    own_cache = [
        pltpu.make_async_copy(
            src.at[:, :, pl.ds(pl.multiple_of(z * HEAD_DIM, HEAD_DIM), HEAD_DIM)],
            rows_recv.at[z, n],
            load_sem.at[len(pairs) + n],
        )
        for n, src in enumerate((key_cache, value_cache))
    ]

    barrier = pltpu.get_barrier_semaphore()
    for t in far_z:
        signal((gx + 4 * (t - z), gy))
    for g in others_of_group:
        signal((4 * z + g, gy))
    for t in others:
        signal((gx, t))
    for half_block in range(2):
        source = 4 * (core * 4 + z // 2) + 2 * yh + half_block

        @pl.when(jnp.logical_and(projects, source != gx))
        def _(source=source):
            signal((source, gy))

    for load in [loads[6], loads[7], loads[9], *own_cache, *loads[1:6], loads[8], lens_load, *loads[10:]]:
        load.start()

    def send(n, src, dst, to):
        pltpu.make_async_remote_copy(
            src_ref=src,
            dst_ref=dst,
            send_sem=send_sem.at[n],
            recv_sem=recv_sem.at[n],
            device_id=to,
            device_id_type=MESH,
        ).start()

    def arrived(n, ref):
        pltpu.make_async_copy(ref, ref, recv_sem.at[n]).wait()

    def sent(n, ref):
        pltpu.make_async_copy(ref, ref, send_sem.at[n]).wait()

    def as_tiles(x, width):
        return [x[:, n * 128 : (n + 1) * 128] for n in range(width // 128)]

    def from_tiles(x):
        return jnp.concatenate([x[:, n, :] for n in range(4)], axis=1)

    loads[0].wait()
    x_send[...] = jnp.concatenate(as_tiles(hid_v[...].astype(F32), 512), axis=0).astype(BF)
    x_recv[z, yh, core] = x_send[...]
    greeted = NZ - 1 + 3 + GY - 1

    @pl.when(keeps_block)
    def _():
        pl.semaphore_wait(barrier, greeted)

    @pl.when(jnp.logical_not(keeps_block))
    def _():
        pl.semaphore_wait(barrier, greeted + 1)

    def over_group(act):
        for g in others_of_group:
            act(g)

    def over_z(act):
        for t in far_z:
            act(t)

    def head_of(t):
        return pl.ds(pl.multiple_of(t * HEAD_DIM, HEAD_DIM), HEAD_DIM)

    three_tiles = x_recv.reshape(GX, 4, 128).at[pl.ds(0, 3)]
    three_rows = cache_recv.reshape(NZ, 4, 2, 8, HEAD_DIM).at[:, pl.ds(0, 3)]

    over_group(lambda g: send(0, x_send, x_recv.at[z, yh, core], (4 * z + g, gy)))
    loads[1].wait()
    loads[2].wait()
    adjusted_in = ah_v[...].astype(F32)
    base_in = bh_v[...].astype(F32)
    sum_adjusted = jnp.sum(adjusted_in * adjusted_in, axis=1, keepdims=True)
    sum_base = jnp.sum(base_in * base_in, axis=1, keepdims=True)
    hidden_in = hid_v[...].astype(F32)
    sum_hidden = jnp.sum(hidden_in * hidden_in, axis=1, keepdims=True)
    sums = (sum_adjusted, sum_base, sum_hidden, sum_hidden)
    st_send[...] = jnp.concatenate([jnp.broadcast_to(t, (1, 128)) for t in sums], axis=0)
    st_recv[gy] = st_send[...]
    for t in others:
        send(1, st_send, st_recv.at[gy], (gx, t))

    loads[6].wait()
    loads[7].wait()
    over_z(
        lambda t: send(2, kv_v.at[:, :, :, head_of(t)], rows_recv.at[z], (gx + 4 * (t - z), gy))
    )
    loads[9].wait()

    @pl.when(keeps_block)
    def _():
        kvw_recv[core] = kvw_v[...]

    @pl.when(jnp.logical_not(keeps_block))
    def _():
        send(12, kvw_v, kvw_recv.at[core], (block_to, gy))

    arrived(0, three_tiles)

    over_z(lambda t: send(13, x_recv.at[z], x_recv.at[z], (gx + 4 * (t - z), gy)))

    def over_gx(act):
        for flip in (1, 0):
            side = 2 * (yh * (1 - flip) + (1 - yh) * flip)
            for to in far_z:
                for c in range(2):
                    act((4 * to + side + c, gy))
        for c in range(2):
            act((4 * z + 2 - 2 * yh + c, gy))
        act((pair + 1 - core, gy))

    arrived(1, st_recv.at[pl.ds(0, GY - 1)])
    totals = jnp.sum(st_recv[...], axis=0)
    loads[3].wait()
    loads[4].wait()
    adjusted = adjusted_in * lax.rsqrt(totals[0:1, 0:1] / D7 + EPS) * agn_v[...]
    base = base_in * lax.rsqrt(totals[1:2, 0:1] / D7 + EPS) * bgn_v[...]
    factor = lax.rsqrt(totals[2:3, :] / D + EPS)
    high = factor.astype(BF).astype(F32)
    ab_send[...] = jnp.concatenate(
        as_tiles(adjusted, 256) + as_tiles(base, 256) + [high, factor - high], axis=0
    ).astype(BF)
    ab_recv[gx] = ab_send[...]
    over_gx(lambda to: send(5, ab_send, ab_recv.at[gx], to))

    for load in own_cache:
        load.wait()
    arrived(2, rows_recv.at[pl.ds(0, NZ - 1)])
    over_group(
        lambda g: send(
            16,
            rows_recv.at[:, :, lax.rem(g, 2)],
            cache_recv.at[:, yh, core],
            (4 * z + g, gy),
        )
    )
    cache_recv[:, yh, core] = rows_recv[:, :, core]

    lane = lax.broadcasted_iota(jnp.int32, (1, HEAD_DIM), 1)
    half = HEAD_DIM // 2
    turn = (lane % half).astype(F32)
    freq = jnp.exp(turn * (-2.0 / HEAD_DIM * math.log(THETA)))
    lens_load.wait()
    length = lens_v[core]
    angle = length.astype(F32) * freq
    cosine = jnp.cos(angle)
    sine = jnp.where(lane < half, -jnp.sin(angle), jnp.sin(angle))

    loads[5].wait()
    loads[8].wait()

    arrived(13, x_recv.at[pl.ds(0, NZ - 1)])
    rows = from_tiles(x_recv[...].astype(F32).reshape(GX, 4, 128))
    scaled = (rows * ag_v[...]).astype(BF)

    @pl.when(projects)
    def _():
        @pl.when(keeps_block)
        def _():
            arrived(12, kvw_recv.at[0])

        @pl.when(jnp.logical_not(keeps_block))
        def _():
            arrived(12, kvw_recv)

        weight = kvw_recv[...].reshape(HEAD_DIM, 512)
        kn_send[...] = times_transposed(scaled, weight).reshape(GX, 1, 128)
        kn_recv[core, gy] = kn_send[row]

        for g in [4 * b + a for b in plane_y[::-1] for a in plane_x]:
            for c in range(2):
                send(15, kn_send.at[2 * g + c], kn_recv.at[core, gy], (4 * z + 2 - 2 * yh + c, g))

    part_q = jnp.dot(scaled, qw_v[...], preferred_element_type=F32)
    q_send[...] = jnp.concatenate(
        [p.reshape(GX, 1, 128) for p in as_tiles(part_q, 256)], axis=1
    ).astype(BF)
    q_recv[row] = q_send[row]

    def over_plane(act):
        for g in others:
            for c in range(2):
                act(c, 2 * g + c, (pair + c, g))
        act(1 - core, 2 * gy + 1 - core, (pair + 1 - core, gy))

    over_plane(lambda c, r, to: send(3, q_send.at[r], q_recv.at[row], to))

    @pl.when(projects)
    def _():
        over_plane(lambda c, r, to: send(4, kn_send.at[r], kn_recv.at[core, gy], to))

    arrived(5, ab_recv.at[pl.ds(0, GX - 1)])
    joined = from_tiles(ab_recv[...].astype(F32)).astype(BF)
    loads[11].wait()
    loads[12].wait()
    part_ab = times_transposed(joined[:, :256], ahead_v[...]) - times_transposed(
        joined[:, 256:], bhead_v[...]
    )
    vocab = part_ab.shape[1]
    for n in range(GY):
        abl_send[n] = part_ab[2 * n : 2 * n + 2]
    abl_recv[gy] = abl_send[gy]
    parts = ab_recv[row].astype(F32)
    factor = parts[4:5, :] + parts[5:6, :]

    arrived(16, three_rows)
    cached = cache_recv[...].reshape(GX, 2, 8, HEAD_DIM).astype(F32)
    keys = cached[:, 0].reshape(CTX, HEAD_DIM).astype(BF)
    values = cached[:, 1].reshape(CTX, HEAD_DIM).astype(BF)

    arrived(3, q_recv.at[pl.ds(0, GX - 1)])
    q_total = jnp.zeros((2, 2, 128), F32)
    for n in range(GY):
        q_total = q_total + q_recv[2 * n : 2 * n + 2].astype(F32)
    query = jnp.concatenate([q_total[0], q_total[1]], axis=0) * factor
    query = query.astype(BF).astype(F32)
    scale = HEAD_DIM ** (-0.5)
    turned = (query * cosine + pltpu.roll(query, half, 1) * sine).astype(BF)
    scores = times_transposed(turned, keys) * scale
    position = lax.broadcasted_iota(jnp.int32, (4, CTX), 1)
    valid = position < length
    scores = jnp.where(valid, scores, NEGATIVE)
    top = jnp.max(scores, axis=1, keepdims=True)

    @pl.when(projects)
    def _():
        arrived(4, kn_recv.reshape(2 * GY, 1, 128).at[pl.ds(0, 2 * GY - 1)])

    @pl.when(jnp.logical_not(projects))
    def _():
        arrived(15, kn_recv)

    fresh_kv = jnp.sum(kn_recv[...], axis=1)
    key_new = (fresh_kv[0] * factor).astype(BF).astype(F32)
    value_new = (fresh_kv[1] * factor).astype(BF).astype(F32)
    fresh_score = jnp.sum(query * key_new, axis=1, keepdims=True) * scale
    top = jnp.maximum(top, fresh_score)
    weights = jnp.where(valid, jnp.exp(scores - top), 0.0)
    fresh = jnp.exp(fresh_score - top)
    total = jnp.sum(weights, axis=1, keepdims=True) + fresh
    summed = jnp.dot(weights.astype(BF), values, preferred_element_type=F32)
    summed = summed + fresh.astype(BF).astype(F32) * value_new
    attn = (summed / total).astype(BF)
    e_send[0] = attn[0:2]
    e_send[1] = attn[2:4]
    e_recv[row] = e_send[core]

    over_plane(lambda c, r, to: send(6, e_send.at[c], e_recv.at[row], to))

    def to_gy(n, src, dst):
        for t in others:
            send(n, src.at[t], dst.at[gy], (gx, t))


    loads[10].wait()
    arrived(6, e_recv.at[pl.ds(0, GX - 1)])
    heads = e_recv[...].astype(F32)
    heads = jnp.concatenate([heads[:, 0, :], heads[:, 1, :]], axis=1).astype(BF)
    mixed = jnp.dot(heads, ow_v[...], preferred_element_type=F32)
    tiles = jnp.concatenate([p.reshape(GX, 1, 128) for p in as_tiles(mixed, 512)], axis=1)
    f_send[...] = tiles.astype(BF).reshape(2, 4, 2, 2, 4, 128)
    z_half, z_in = z // 4, z % 4
    slot = 2 * z_in + core
    f_recv[slot] = f_send[:, z_in, :, core]

    for to in (3 - z_in, lax.rem(z_in + 2, 4), z_in + 1 - 2 * (z_in % 2)):
        for c in range(2):
            there = (4 * (4 * z_half + to) + 2 * yh + c, gy)
            send(8, f_send.at[:, to, :, c], f_recv.at[slot], there)
    send(8, f_send.at[:, z_in, :, 1 - core], f_recv.at[slot], (pair + 1 - core, gy))
    to_gy(7, abl_send, abl_recv)
    loads[13].wait()
    loads[14].wait()
    own_rows = x_recv.reshape(2, 4, 2, 2, 4, 128)[:, z_in, :, core].astype(F32)
    quarter = 2 * z_half + yh
    own_rows = own_rows * jnp.where(quarter == 0, 1.0, 0.0)
    arrived(8, f_recv.at[pl.ds(0, 7)])
    partial = jnp.sum(f_recv[...].astype(F32), axis=0)

    h_send[...] = (partial + own_rows).astype(BF)
    h_recv[quarter, :, z_in, :, core] = h_send[...]
    over_gx(lambda to: send(9, h_send, h_recv.at[quarter, :, z_in, :, core], to))
    arrived(7, abl_recv.at[pl.ds(0, GY - 1)])
    ab_logits = jnp.sum(abl_recv[...], axis=0)
    arrived(9, h_recv.reshape(GX, 4, 4, 128).at[pl.ds(0, GX - 1)])
    rows = from_tiles(jnp.sum(h_recv[...].astype(F32), axis=0).reshape(GX, 4, 128))
    squares = jnp.sum(rows * rows, axis=1, keepdims=True)
    scaled = (rows * fg_v[...]).astype(BF)
    part = times_transposed(scaled, h70_v[...])
    high = squares.astype(BF).astype(F32)
    low = squares - high
    rest = (WIDTH - vocab) // 2
    tail = [jnp.broadcast_to(high, (GX, rest)), jnp.broadcast_to(low, (GX, rest))]
    part = jnp.concatenate([part, *tail], axis=1).astype(BF)
    for n in range(GY):
        i_send[n] = part[2 * n : 2 * n + 2]
    i_recv[gy] = i_send[gy]

    to_gy(10, i_send, i_recv)
    arrived(10, i_recv.at[pl.ds(0, GY - 1)])
    summed = jnp.sum(i_recv[...].astype(F32), axis=0)
    square = summed[:, vocab : vocab + 1] + summed[:, WIDTH - 1 :]
    factor = lax.rsqrt(square / D + EPS)
    logits = summed[:, :vocab] * factor + ab_logits
    peak = jnp.max(logits, axis=1, keepdims=True)
    partial_lse = peak + jnp.log(jnp.sum(jnp.exp(logits - peak), axis=1, keepdims=True))
    j_send[...] = jnp.broadcast_to(partial_lse, (2, 128))
    j_recv[gx] = j_send[...]

    over_gx(lambda to: send(11, j_send, j_recv.at[gx], to))
    arrived(11, j_recv.at[pl.ds(0, GX - 1)])
    everyone = j_recv[...]
    peak = jnp.max(everyone, axis=0)
    lse = peak + jnp.log(jnp.sum(jnp.exp(everyone - peak[None]), axis=0))
    out[...] = logits - lse[:, 0:1]

    sent(0, three_tiles)
    sent(1, st_recv.at[pl.ds(0, GY - 1)])
    sent(2, rows_recv.at[pl.ds(0, NZ - 1)])
    sent(3, q_recv.at[pl.ds(0, GX - 1)])

    @pl.when(projects)
    def _():
        sent(15, kn_send)
        sent(4, kn_send.at[pl.ds(0, GX - 1)])

    sent(5, ab_recv.at[pl.ds(0, GX - 1)])
    sent(6, e_recv.at[pl.ds(0, GX - 1)])
    sent(7, abl_recv.at[pl.ds(0, GY - 1)])
    sent(8, f_recv.at[pl.ds(0, 7)])
    sent(9, h_recv.reshape(GX, 4, 4, 128).at[pl.ds(0, GX - 1)])
    sent(10, i_recv.at[pl.ds(0, GY - 1)])
    sent(11, j_recv.at[pl.ds(0, GX - 1)])

    @pl.when(jnp.logical_not(keeps_block))
    def _():
        sent(12, kvw_v)

    sent(13, x_recv.at[pl.ds(0, NZ - 1)])
    sent(16, three_rows)


def body(
    hidden70,
    attn_gain,
    final_gain,
    query_weight,
    keyvalue_weight,
    out_weight,
    key_cache,
    value_cache,
    lengths,
    head70,
    adjusted_hidden,
    adjusted_gain,
    adjusted_head,
    base_hidden,
    base_gain,
    base_head,
):
    vocab = head70.shape[1]
    operands = (
        hidden70,
        attn_gain.reshape(1, -1),
        final_gain.reshape(1, -1),
        query_weight,
        keyvalue_weight.T,
        out_weight,
        key_cache,
        value_cache,
        head70.T,
        adjusted_hidden,
        adjusted_gain.reshape(1, -1),
        adjusted_head.T,
        base_hidden,
        base_gain.reshape(1, -1),
        base_head.T,
    )

    def like(a):
        return pltpu.VMEM(a.shape, a.dtype)

    caches = pltpu.VMEM((2, *key_cache.shape), BF)
    local = [like(a) for a in operands[:6]] + [caches] + [like(a) for a in operands[8:]]
    vm = pltpu.VMEM
    exchange = [
        vm((4, 128), BF),
        vm((NZ, 2, 2, 4, 128), BF),
        vm((4, 128), F32),
        vm((GY, 4, 128), F32),
        vm((2, 64, 512), BF),
        vm((NZ, 2, 2, 8, HEAD_DIM), BF),
        vm((NZ, 2, 2, 2, 8, 128), BF),
        vm((6, 128), BF),
        vm((GX, 6, 128), BF),
        vm((GX, 2, 128), BF),
        vm((GX, 2, 128), BF),
        vm((GX, 1, 128), F32),
        vm((2, GY, 1, 128), F32),
        vm((2, 2, 128), BF),
        vm((GX, 2, 128), BF),
        vm((2, 4, 2, 2, 4, 128), BF),
        vm((8, 2, 2, 4, 128), BF),
        vm((2, 2, 4, 128), BF),
        vm((4, 2, 4, 2, 2, 4, 128), BF),
        vm((GY, 2, vocab), F32),
        vm((GY, 2, vocab), F32),
        vm((GY, 2, WIDTH), BF),
        vm((GY, 2, WIDTH), BF),
        vm((2, 128), F32),
        vm((GX, 2, 128), F32),
    ]
    return pl.pallas_call(
        kernel,
        out_shape=pltpu.VMEM((2, vocab), F32),
        in_specs=[pl.BlockSpec(memory_space=pl.ANY)] * (1 + len(operands)),
        out_specs=pl.BlockSpec(memory_space=pltpu.VMEM),
        scratch_shapes=local
        + [pltpu.SMEM(lengths.shape, lengths.dtype)]
        + exchange
        + [
            pltpu.SemaphoreType.DMA((18,)),
            pltpu.SemaphoreType.DMA((17,)),
            pltpu.SemaphoreType.DMA((17,)),
        ],
        compiler_params=pltpu.CompilerParams(collective_id=0, has_side_effects=True),
    )(lengths, *operands)


def solution(mesh):
    placed = (
        P("gx", "gy"),
        P("gy"),
        P("gy"),
        P("gy", "gx"),
        P("gy", "gx"),
        P("gx", "gy"),
        P("gy", "gx", None),
        P("gy", "gx", None),
        P("gy"),
        P("gy", "gx"),
        P("gx", "gy"),
        P("gy"),
        P("gy", "gx"),
        P("gx", "gy"),
        P("gy"),
        P("gy", "gx"),
    )
    return jax.shard_map(body, mesh=mesh, in_specs=placed, out_specs=P("gy", "gx"), check_vma=False)
```
